32 devices in a mesh: parts: 2 (over x), frame: 2 (over core), tile: 8 (over z, y).
Axes of the slice: x: 2, y: 2, z: 4, core: 2. Of those that a mesh axis runs over, the one named last changes fastest.
Arguments:
- decoded_refs: bfloat16 [64, 96, 64, 256], P(('parts', 'frame'), None, 'tile'), parts along dimension 0, may hold values from -6 to 6
- current_frames: bfloat16 [16, 96, 64, 256], P(('parts', 'frame'), None, 'tile'), parts along dimension 0, may hold values from -6 to 6
- ref_pairs: int32 [16, 2], P('parts'), parts along dimension 0, may hold values from 0 to 31
- ref_slots: int32 [64], P('parts'), parts along dimension 0, may hold values from 0 to 31, each once
- frame_numbers: int32 [16], P('parts'), parts along dimension 0, may hold values from 0 to 31
- rate_weights: float32 [64], P('parts'), parts along dimension 0, may hold values from 0.5 to 4
- join_kernel: bfloat16 [3, 3, 96, 288], replicated, may hold values from -0.125 to 0.125
- out_kernel: bfloat16 [3, 3, 96, 96], replicated, may hold values from -0.21875 to 0.21875
Outputs:
- reconstruction: bfloat16 [16, 96, 64, 256], P(('parts', 'frame'), None, 'tile'), parts along dimension 0
- join_grad: float32 [6, 3, 96, 288], P('parts'), parts along dimension 0
- output_grad: float32 [6, 3, 96, 96], P('parts'), parts along dimension 0
The draws below stay inside these ranges and needn't reach their ends.
There are 2 independent parts, one for each index of `parts`. The reference program is written for one: setup_inputs(seed, part) draws one part's arguments, and reference() takes and returns one part's arrays. A program takes and returns all parts, laid end to end along the dimension named above; an argument that names none is the same for every part. Nothing has to cross between parts.
Inputs may be any that keep to these rules, and one draw needn't show every extreme that they name: `ref_pairs`: each B-frame names two decoded frames, possibly the same one. `ref_slots`: each slot holds exactly one decoded frame.
All inputs are finite; a program needn't handle non-finite values.
Results may differ from the reference program's by a relative error of at most 0.005.
Values may be sent and summed in bfloat16 or wider, within the bound.
No kernel may reach another device: no remote copies, remote signals or barrier semaphores. Data moves between devices by JAX's collectives and lax.ppermute only.
A program may use at most 128 MiB of HBM per device.

```python
import math
import jax
import jax.numpy as jnp
from jax import lax

C = 96
COLS = 256
NB = 8
NREF = 32
GOP = 32
H = 64


def set_ends(array, stream_key, smallest, top_value):
    index_at = [jax.random.randint(jax.random.fold_in(stream_key, axis), (), 0, length) for axis, length in enumerate(array.shape)]
    main_axis = array.shape.index(max(array.shape))
    next_to = index_at[:main_axis] + [(index_at[main_axis] + 1) % array.shape[main_axis]] + index_at[main_axis + 1:]
    return array.at[tuple(index_at)].set(smallest).at[tuple(next_to)].set(top_value)


def levels(rng, shape, cuts, least, top_value):
    gain, own = 1.0, jax.random.fold_in(rng, 6)
    for dim, blocks in cuts:
        draws = jnp.exp(jax.random.uniform(jax.random.fold_in(own, dim), (blocks,), jnp.float32, least / len(cuts), top_value / len(cuts)))
        gain = gain * jnp.repeat(draws, shape[dim] // blocks).reshape([-1 if axis == dim else 1 for axis in range(len(shape))])
    return gain


def centred(own_key, shape, deviation, bound, split=(), held_as=jnp.bfloat16):
    entries = deviation * jax.random.normal(own_key, shape, jnp.float32)
    if split:
        entries = entries * levels(own_key, shape, split, -0.22, 0.18)
    return jnp.clip(entries, -bound, bound).astype(held_as)


def setup_inputs(seed: int = 0, part: int = 0) -> dict:
    splits = jax.random.split(jax.random.key(seed), 9)
    own_keys = jax.random.split(jax.random.fold_in(splits[8], part), 9)
    return {
        "decoded_refs": centred(own_keys[0], (NREF, C, H, COLS), 1.0, 6.0, ((0, 2), (2, 8))),
        "current_frames": centred(own_keys[1], (NB, C, H, COLS), 1.0, 6.0, ((0, 2), (2, 8))),
        "ref_pairs": set_ends(jax.random.randint(own_keys[2], (NB, 2), 0, NREF), jax.random.fold_in(own_keys[2], 1), 0, NREF - 1).astype(jnp.int32),
        "ref_slots": jax.random.permutation(own_keys[3], NREF).astype(jnp.int32),
        "frame_numbers": set_ends(jax.random.randint(own_keys[4], (NB,), 0, GOP), jax.random.fold_in(own_keys[4], 1), 0, GOP - 1).astype(jnp.int32),
        "rate_weights": jnp.clip(jnp.exp(jax.random.uniform(own_keys[5], (GOP,), jnp.float32, math.log(0.5), math.log(4.0))), 0.5, 4.0),
        "join_kernel": centred(splits[6], (3, 3, C, 3 * C), (27 * C) ** -0.5, 0.125),
        "out_kernel": centred(splits[7], (3, 3, C, C), (9 * C) ** -0.5, 0.21875),
    }


def sigmoid_grad(value):
    sigma = jax.nn.sigmoid(value)
    return sigma * (1.0 + value * (1.0 - sigma))

def apply_taps(padded, kernel, row_count, col_count):
    running = jnp.zeros((kernel.shape[2], row_count, col_count), jnp.float32)
    for row_tap in range(3):
        for col_tap in range(3):
            window = padded[:, row_tap:row_tap + row_count, col_tap:col_tap + col_count]
            running = running + jnp.einsum('oi,ihw->ohw', kernel[row_tap, col_tap], window)
    return running

def tap_grads(upstream, padded, row_count, col_count):
    pieces = []
    for row_tap in range(3):
        for col_tap in range(3):
            window = padded[:, row_tap:row_tap + row_count, col_tap:col_tap + col_count]
            pieces.append(jnp.einsum('ohw,ihw->oi', upstream, window))
    stacked = jnp.stack(pieces)
    return stacked.reshape((3, 3) + stacked.shape[1:])

def pad_frame(field):
    return jnp.pad(field, ((0, 0), (1, 1), (1, 1)))

def reference(decoded_refs, current_frames, ref_pairs, ref_slots, frame_numbers, rate_weights, join_kernel, out_kernel):
    row_count = current_frames.shape[2]
    col_count = current_frames.shape[3]
    join_full = join_kernel.astype(jnp.float32)
    out_full = out_kernel.astype(jnp.float32)

    def frame_step(index):
        slot_ids = ref_slots[ref_pairs[index]]
        stacked = jnp.concatenate([decoded_refs[slot_ids[0]], decoded_refs[slot_ids[1]], current_frames[index]], 0)
        stacked_pad = pad_frame(stacked.astype(jnp.float32))
        preact = apply_taps(stacked_pad, join_full, row_count, col_count)
        hidden = jax.nn.silu(preact).astype(jnp.bfloat16)
        hidden = lax.optimization_barrier(hidden).astype(jnp.float32)
        hidden_pad = pad_frame(hidden)
        recon = apply_taps(hidden_pad, out_full, row_count, col_count)
        rate_weight = rate_weights[frame_numbers[index]]
        residual = (2.0 * rate_weight * (recon - current_frames[index].astype(jnp.float32)) / (row_count * col_count)).astype(jnp.bfloat16)
        residual = lax.optimization_barrier(residual).astype(jnp.float32)
        output_part = tap_grads(residual, hidden_pad, row_count, col_count)
        residual_pad = pad_frame(residual)
        hidden_grad = jnp.zeros((out_full.shape[3], row_count, col_count), jnp.float32)
        for row_tap in range(3):
            for col_tap in range(3):
                window = residual_pad[:, 2 - row_tap:2 - row_tap + row_count, 2 - col_tap:2 - col_tap + col_count]
                hidden_grad = hidden_grad + jnp.einsum('oi,ohw->ihw', out_full[row_tap, col_tap], window)
        preact_grad = (hidden_grad * sigmoid_grad(preact)).astype(jnp.bfloat16)
        preact_grad = lax.optimization_barrier(preact_grad).astype(jnp.float32)
        join_part = tap_grads(preact_grad, stacked_pad, row_count, col_count)
        return (recon.astype(jnp.bfloat16), join_part, output_part)
    recon_all, join_parts, output_parts = lax.map(frame_step, jnp.arange(current_frames.shape[0], dtype=jnp.int32))
    return (recon_all, lax.optimization_barrier(jnp.sum(join_parts, 0)), lax.optimization_barrier(jnp.sum(output_parts, 0)))
```

```python
import functools

import jax
import jax.numpy as jnp
from jax import lax
from jax.experimental import pallas as pl
from jax.experimental.pallas import tpu as pltpu
from jax.sharding import PartitionSpec as P

F32 = jnp.float32
BF16 = jnp.bfloat16
LANES = 128


def call(body, name, flops, nbytes, **kw):
    return pl.pallas_call(
        body,
        name=name,
        cost_estimate=pl.CostEstimate(flops=flops, bytes_accessed=nbytes, transcendentals=0),
        compiler_params=pltpu.CompilerParams(vmem_limit_bytes=40 * 1024 * 1024),
        **kw,
    )


def frame_spec(shape):
    return pl.BlockSpec((1,) + shape[1:], lambda b: (b,) + (0,) * (len(shape) - 1))


def whole_spec(shape):
    return pl.BlockSpec(shape, lambda *_: (0,) * len(shape))


def from_left(x):
    lane = lax.broadcasted_iota(jnp.int32, x.shape, 1)
    return jnp.where(lane == 0, jnp.zeros((), x.dtype), pltpu.roll(x, 1, 1))


def from_right(x):
    lane = lax.broadcasted_iota(jnp.int32, x.shape, 1)
    w = x.shape[1]
    return jnp.where(lane == w - 1, jnp.zeros((), x.dtype), pltpu.roll(x, w - 1, 1))


def shift_sum(y):
    c = y.shape[0] // 3
    return y[c : 2 * c] + from_left(y[:c]) + from_right(y[2 * c :])


def conv_rows(weights, rows, width, group=2):
    zero = jnp.zeros_like(rows[0])
    padded = [zero] + rows + [zero]
    sums = []
    for r0 in range(0, len(rows), group):
        columns = [
            jnp.concatenate(padded[r : r + 3], 0) for r in range(r0, min(r0 + group, len(rows)))
        ]
        y = jnp.dot(weights, jnp.concatenate(columns, 1), preferred_element_type=F32)
        for j in range(len(columns)):
            sums.append(shift_sum(y[:, j * width : (j + 1) * width]))
    return sums


def gather_body(pairs, slots, group, refs, out):
    out[...] = refs[...]


def edge_taps_body(xr0, xc0, xr1, xc1, w, up, down):
    frames = up.shape[0]
    for xr, xc, tap, out in ((xr0, xc0, 1, up), (xr1, xc1, 0, down)):
        for b in range(frames):
            x = jnp.concatenate([xr[b, 0], xc[b, 0]], 0)
            y = jnp.dot(w[tap], x, preferred_element_type=F32)
            out[b] = shift_sum(y).astype(BF16)


def silu_and_slope(v):
    s = jax.nn.sigmoid(v)
    return (v * s).astype(BF16), s * (1.0 + v * (1.0 - s))


def join_body(xr, xc, w, hidden, slope, edge):
    rows, width = xr.shape[1], xr.shape[3]
    stacked = [jnp.concatenate([xr[0, r], xc[0, r]], 0) for r in range(rows)]
    sums = conv_rows(w[...], stacked, width)
    edge[0, 0] = sums[0]
    edge[0, 1] = sums[-1]
    for r in range(1, rows - 1):
        hidden[0, r - 1], slope[0, r - 1] = silu_and_slope(sums[r])


def join_edge_body(edge, above, below, hidden, slope):
    for b in range(edge.shape[0]):
        for k, got in enumerate((above, below)):
            hidden[b, k], slope[b, k] = silu_and_slope(edge[b, k] + got[b].astype(F32))


def frame_scale(pairs, cells, b, frames):
    numbers, rates, group = pairs
    return rates[numbers[group[0] * frames + b]] * (2.0 / cells)


def output_body(numbers, rates, group, hm, he, xc, w, recon, residual, edge, *, cells, frames):
    rows, width = hm.shape[1] + 2, hm.shape[3]
    hidden = [he[0, 0]] + [hm[0, r] for r in range(rows - 2)] + [he[0, 1]]
    sums = conv_rows(w[...], hidden, width)
    scale = frame_scale((numbers, rates, group), cells, pl.program_id(0), frames)
    edge[0, 0] = sums[0]
    edge[0, 1] = sums[-1]
    for r in range(1, rows - 1):
        recon[0, r - 1] = sums[r].astype(BF16)
        residual[0, r - 1] = ((sums[r] - xc[0, r].astype(F32)) * scale).astype(BF16)


def output_edge_body(
    numbers, rates, group, edge, above, below, xc0, xc1, w, recon, residual, *, cells, frames
):
    for b in range(edge.shape[0]):
        scale = frame_scale((numbers, rates, group), cells, b, frames)
        for k, (got, xc) in enumerate(((above, xc0), (below, xc1))):
            y = jnp.dot(w[k], got[b], preferred_element_type=F32)
            total = edge[b, k] + shift_sum(y)
            recon[b, k] = total.astype(BF16)
            residual[b, k] = ((total - xc[b, 0].astype(F32)) * scale).astype(BF16)


def slope_body(rm, re, slope, w, grad, edge):
    rows, width = rm.shape[1] + 2, rm.shape[3]
    residual = [re[0, 0]] + [rm[0, r] for r in range(rows - 2)] + [re[0, 1]]
    sums = conv_rows(w[...], residual, width)
    edge[0, 0] = sums[0]
    edge[0, 1] = sums[-1]
    for r in range(1, rows - 1):
        grad[0, r - 1] = (sums[r] * slope[0, r - 1]).astype(BF16)


def slope_edge_body(edge, above, below, slope, w, grad):
    for b in range(edge.shape[0]):
        for k, got in enumerate((above, below)):
            y = jnp.dot(w[k], got[b], preferred_element_type=F32)
            grad[b, k] = ((edge[b, k] + shift_sum(y)) * slope[b, k]).astype(BF16)


def contract(left, right):
    return lax.dot_general(left, right, (((1,), (1,)), ((), ())), preferred_element_type=F32)


def lane_blocks(x):
    return [x[:, k : k + LANES] for k in range(0, x.shape[1], LANES)]


def grads_body(gm, ge, xr, xc, hm, he, rm, re, above, below, packed):
    rows, width = gm.shape[1] + 2, gm.shape[3]
    channels = gm.shape[2]
    joined = xr.shape[2] + xc.shape[2]
    rest = joined % 256
    head = joined - rest
    zero = jnp.zeros((channels, width), BF16)
    grad = [ge[0, 0]] + [gm[0, r] for r in range(rows - 2)] + [ge[0, 1]]
    turned = [[from_right(g) for g in grad], grad, [from_left(g) for g in grad]]
    stacked = [jnp.concatenate([xr[0, r], xc[0, r]], 0) for r in range(rows)]
    taps = []
    for p in range(3):
        for q in range(3):
            taps.append(
                jnp.concatenate(
                    [turned[q][r - p + 1] if 0 <= r - p + 1 < rows else zero for r in range(rows)],
                    1,
                )
            )
    main = contract(
        jnp.concatenate(taps, 0), jnp.concatenate([s[:head] for s in stacked], 1)
    )
    tails = [s[head:] for s in stacked]
    tail_zero = jnp.zeros_like(tails[0])
    tail = contract(
        jnp.concatenate([jnp.concatenate(turned[q], 1) for q in range(3)], 0),
        jnp.concatenate(
            [
                jnp.concatenate(
                    [tails[r + p - 1] if 0 <= r + p - 1 < rows else tail_zero for r in range(rows)],
                    1,
                )
                for p in range(3)
            ],
            0,
        ),
    )
    hidden = [he[0, 0]] + [hm[0, r] for r in range(rows - 2)] + [he[0, 1]]
    shifted = [[from_left(h) for h in hidden], hidden, [from_right(h) for h in hidden]]
    residual = (
        [above[0], re[0, 0]] + [rm[0, r] for r in range(rows - 2)] + [re[0, 1], below[0]]
    )
    out = contract(
        jnp.concatenate(
            [jnp.concatenate([residual[r - p + 2] for r in range(rows)], 1) for p in range(3)], 0
        ),
        jnp.concatenate([jnp.concatenate(shifted[q], 1) for q in range(3)], 0),
    )
    blocks = lane_blocks(main) + lane_blocks(jnp.concatenate([out, tail], 1))
    first = pl.program_id(0) == 0

    @pl.when(first)
    def _():
        at = 0
        for block in blocks:
            packed[at : at + block.shape[0], :] = block
            at += block.shape[0]
        if at < packed.shape[0]:
            packed[at:, :] = jnp.zeros((packed.shape[0] - at, LANES), F32)

    @pl.when(jnp.logical_not(first))
    def _():
        at = 0
        for block in blocks:
            packed[at : at + block.shape[0], :] += block
            at += block.shape[0]


def grads_edge_body(packed_in, above, below, xr0, xc0, xr1, xc1, packed):
    frames, channels, _ = above.shape
    joined = xr0.shape[2] + xc0.shape[2]
    rest = joined % 256
    head = joined - rest
    taps = 3 * channels
    packed[...] = packed_in[...]
    tail_at = 3 * taps * (head // LANES)
    tail_lane = taps
    for p, got, xr, xc in ((2, above, xr0, xc0), (0, below, xr1, xc1)):
        rows = [got[b] for b in range(frames)]
        left = jnp.concatenate(
            [
                jnp.concatenate([move(g) for g in rows], 1)
                for move in (from_right, lambda g: g, from_left)
            ],
            0,
        )
        right = jnp.concatenate(
            [jnp.concatenate([xr[b, 0], xc[b, 0]], 0) for b in range(frames)], 1
        )
        extra = contract(left, right)
        for k, block in enumerate(lane_blocks(extra[:, :head])):
            at = 3 * taps * k + taps * p
            packed[at : at + taps, :] += block
        lane = tail_lane + rest * p
        at = tail_at + taps * (lane // LANES)
        lane = lane % LANES
        packed[at : at + taps, lane : lane + rest] += extra[:, head:]


def unpack_body(packed, join, out):
    channels = out.shape[2]
    joined = join.shape[3]
    rest = joined % 256
    head = joined - rest
    taps = 3 * channels
    tail_at = 3 * taps * (head // LANES)
    tail = jnp.concatenate(
        [
            packed[tail_at + taps * k : tail_at + taps * (k + 1), :]
            for k in range((taps + 3 * rest) // LANES)
        ],
        1,
    )
    for p in range(3):
        for q in range(3):
            rows = slice(q * channels, (q + 1) * channels)
            pieces = [
                packed[
                    3 * taps * k + taps * p + q * channels : 3 * taps * k
                    + taps * p
                    + (q + 1) * channels,
                    :,
                ]
                for k in range(head // LANES)
            ]
            pieces.append(tail[rows, taps + rest * p : taps + rest * (p + 1)])
            join[p, q] = jnp.concatenate(pieces, 1)
            out[p, q] = tail[p * channels : (p + 1) * channels, q * channels : (q + 1) * channels]


def swap_edges(up, down, axis):
    count = lax.axis_size(axis)
    ends = count - 1
    below = lax.ppermute(up, axis, [(i + 1, i) for i in range(ends)])
    above = lax.ppermute(down, axis, [(i, i + 1) for i in range(ends)])
    return above, below


def reduce_all(packed, steps):
    part = packed
    for axis, stride in steps:
        count = lax.axis_size(axis)
        bit = (lax.axis_index(axis) // stride) % 2
        half = part.shape[0] // 2
        send = lax.dynamic_slice_in_dim(part, (1 - bit) * half, half, 0)
        keep = lax.dynamic_slice_in_dim(part, bit * half, half, 0)
        part = keep + lax.ppermute(send, axis, [(i, i ^ stride) for i in range(count)])
    for axis, stride in reversed(steps):
        count = lax.axis_size(axis)
        bit = (lax.axis_index(axis) // stride) % 2
        got = lax.ppermute(part, axis, [(i, i ^ stride) for i in range(count)])
        part = jnp.concatenate(
            [jnp.where(bit == 0, part, got), jnp.where(bit == 0, got, part)], 0
        )
    return part


def on_device(
    decoded_refs,
    current_frames,
    ref_pairs,
    ref_slots,
    frame_numbers,
    rate_weights,
    join_kernel,
    out_kernel,
):
    local_refs = decoded_refs.shape[0]
    frames, channels, rows, width = current_frames.shape
    joined = join_kernel.shape[3]
    cells = rows * lax.axis_size("tile") * width
    group = lax.axis_index("frame")
    group_id = group.reshape(1).astype(jnp.int32)
    picks = 2 * frames
    taps = 3 * channels
    conv_flops = 2 * frames * rows * width * 3 * taps

    def gathered(owner, name):
        tile = decoded_refs.shape[1:]

        def tile_at(i, pairs, slots, ids):
            wanted = (ids[0] if owner == 0 else 1 - ids[0]) * frames + i // 2
            slot = slots[pairs[wanted * 2 + i % 2]] - ids[0] * local_refs
            return (jnp.clip(slot, 0, local_refs - 1), 0, 0, 0)

        return call(
            gather_body,
            name,
            0,
            4 * picks * channels * rows * width,
            grid_spec=pltpu.PrefetchScalarGridSpec(
                num_scalar_prefetch=3,
                grid=(picks,),
                in_specs=[pl.BlockSpec((1,) + tile, tile_at)],
                out_specs=pl.BlockSpec((1,) + tile, lambda i, *_: (i, 0, 0, 0)),
            ),
            out_shape=jax.ShapeDtypeStruct((picks,) + tile, BF16),
        )(ref_pairs.reshape(-1), ref_slots, group_id, decoded_refs)

    outgoing = gathered(1, "gather_out")
    incoming = lax.ppermute(outgoing, "frame", [(0, 1), (1, 0)])
    own = gathered(0, "gather_own")
    pairs = lax.dynamic_slice_in_dim(ref_pairs, group * frames, frames, 0)
    slot_range = jnp.arange(ref_slots.shape[0], dtype=jnp.int32)
    slots = jnp.sum(jnp.where(pairs[:, :, None] == slot_range, ref_slots, 0), axis=-1)
    held = slots // local_refs == group
    picked = jnp.where(
        held[:, :, None, None, None],
        own.reshape(frames, 2, channels, rows, width),
        incoming.reshape(frames, 2, channels, rows, width),
    )
    xr = picked.transpose(0, 3, 1, 2, 4).reshape(frames, rows, 2 * channels, width)
    xc = current_frames.transpose(0, 2, 1, 3)

    join_w = join_kernel.transpose(1, 2, 0, 3).reshape(taps, 3 * joined)
    join_edge_w = join_kernel[0::2].reshape(2, taps, joined)
    out_w = out_kernel.transpose(1, 2, 0, 3).reshape(taps, taps)
    out_edge_w = out_kernel[0::2].reshape(2, taps, channels)
    back = out_kernel[::-1, ::-1].transpose(0, 1, 3, 2)
    back_w = back.transpose(1, 2, 0, 3).reshape(taps, taps)
    back_edge_w = back[0::2].reshape(2, taps, channels)

    mid = (frames, rows - 2, channels, width)
    ends = (frames, 2, channels, width)
    line = (frames, channels, width)

    def struct(shape, dtype):
        return jax.ShapeDtypeStruct(shape, dtype)

    def row_spec(x, r):
        shape = (frames, 1) + x.shape[2:]
        return pl.BlockSpec(shape, lambda *_: (0, r, 0, 0))

    up, down = call(
        edge_taps_body,
        "edge_taps",
        conv_flops * joined // (3 * rows) * 2,
        8 * frames * joined * width,
        grid=(1,),
        in_specs=[
            row_spec(xr, 0),
            row_spec(xc, 0),
            row_spec(xr, rows - 1),
            row_spec(xc, rows - 1),
            whole_spec(join_edge_w.shape),
        ],
        out_specs=[whole_spec(line)] * 2,
        out_shape=[struct(line, BF16)] * 2,
    )(xr, xc, xr, xc, join_edge_w)
    above, below = swap_edges(up, down, "tile")

    hm, sm, pe = call(
        join_body,
        "join_conv",
        conv_flops * joined,
        frames * rows * width * (2 * joined + 6 * channels),
        grid=(frames,),
        in_specs=[frame_spec(xr.shape), frame_spec(xc.shape), whole_spec(join_w.shape)],
        out_specs=[frame_spec(mid), frame_spec(mid), frame_spec(ends)],
        out_shape=[struct(mid, BF16), struct(mid, F32), struct(ends, F32)],
    )(xr, xc, join_w)

    he, se = call(
        join_edge_body,
        "join_edge",
        10 * frames * 2 * channels * width,
        14 * frames * 2 * channels * width,
        grid=(1,),
        in_specs=[whole_spec(ends), whole_spec(line), whole_spec(line)],
        out_specs=[whole_spec(ends)] * 2,
        out_shape=[struct(ends, BF16), struct(ends, F32)],
    )(pe, above, below)
    h_above, h_below = swap_edges(he[:, 0], he[:, 1], "tile")

    rated = (frame_numbers, rate_weights, group_id)
    cm, rm, ce = call(
        functools.partial(output_body, cells=cells, frames=frames),
        "out_conv",
        conv_flops * channels,
        frames * rows * width * 8 * channels,
        grid_spec=pltpu.PrefetchScalarGridSpec(
            num_scalar_prefetch=3,
            grid=(frames,),
            in_specs=[
                pl.BlockSpec((1,) + s[1:], lambda b, *_: (b, 0, 0, 0))
                for s in (mid, ends, xc.shape)
            ]
            + [whole_spec(out_w.shape)],
            out_specs=[
                pl.BlockSpec((1,) + s[1:], lambda b, *_: (b, 0, 0, 0)) for s in (mid, mid, ends)
            ],
        ),
        out_shape=[struct(mid, BF16), struct(mid, BF16), struct(ends, F32)],
    )(*rated, hm, he, xc, out_w)

    ce, re = call(
        functools.partial(output_edge_body, cells=cells, frames=frames),
        "out_edge",
        conv_flops * channels // (3 * rows) * 2,
        14 * frames * 2 * channels * width,
        grid_spec=pltpu.PrefetchScalarGridSpec(
            num_scalar_prefetch=3,
            grid=(1,),
            in_specs=[
                whole_spec(ends),
                whole_spec(line),
                whole_spec(line),
                row_spec(xc, 0),
                row_spec(xc, rows - 1),
                whole_spec(out_edge_w.shape),
            ],
            out_specs=[whole_spec(ends)] * 2,
        ),
        out_shape=[struct(ends, BF16)] * 2,
    )(*rated, ce, h_above, h_below, xc, xc, out_edge_w)
    r_above, r_below = swap_edges(re[:, 0], re[:, 1], "tile")

    gm, de = call(
        slope_body,
        "back_conv",
        conv_flops * channels,
        frames * rows * width * 8 * channels,
        grid=(frames,),
        in_specs=[frame_spec(mid), frame_spec(ends), frame_spec(mid), whole_spec(back_w.shape)],
        out_specs=[frame_spec(mid), frame_spec(ends)],
        out_shape=[struct(mid, BF16), struct(ends, F32)],
    )(rm, re, sm, back_w)

    ge = call(
        slope_edge_body,
        "back_edge",
        conv_flops * channels // (3 * rows) * 2,
        14 * frames * 2 * channels * width,
        grid=(1,),
        in_specs=[
            whole_spec(ends),
            whole_spec(line),
            whole_spec(line),
            whole_spec(ends),
            whole_spec(back_edge_w.shape),
        ],
        out_specs=whole_spec(ends),
        out_shape=struct(ends, BF16),
    )(de, r_above, r_below, se, back_edge_w)
    g_above, g_below = swap_edges(ge[:, 0], ge[:, 1], "tile")

    steps = [("frame", 1)]
    stride = 1
    while stride < lax.axis_size("tile"):
        steps.append(("tile", stride))
        stride *= 2
    unit = 8 << len(steps)
    packed_rows = 3 * taps * (joined + channels) // LANES
    packed_shape = (pl.cdiv(packed_rows, unit) * unit, LANES)
    packed = call(
        grads_body,
        "grads",
        conv_flops * (joined + channels),
        frames * rows * width * (2 * joined + 6 * channels),
        grid=(frames,),
        in_specs=[
            frame_spec(x.shape) for x in (gm, ge, xr, xc, hm, he, rm, re, r_above, r_below)
        ],
        out_specs=whole_spec(packed_shape),
        out_shape=struct(packed_shape, F32),
    )(gm, ge, xr, xc, hm, he, rm, re, r_above, r_below)
    packed = call(
        grads_edge_body,
        "grads_edge",
        conv_flops * joined // (3 * rows) * 2,
        8 * packed_shape[0] * LANES,
        grid=(1,),
        in_specs=[
            whole_spec(packed_shape),
            whole_spec(line),
            whole_spec(line),
            row_spec(xr, 0),
            row_spec(xc, 0),
            row_spec(xr, rows - 1),
            row_spec(xc, rows - 1),
        ],
        out_specs=whole_spec(packed_shape),
        out_shape=struct(packed_shape, F32),
        input_output_aliases={0: 0},
    )(packed, g_above, g_below, xr, xc, xr, xc)
    total = reduce_all(packed, steps)
    join_total, out_total = call(
        unpack_body,
        "unpack",
        0,
        8 * packed_shape[0] * LANES,
        grid=(1,),
        in_specs=[whole_spec(packed_shape)],
        out_specs=[whole_spec(join_kernel.shape), whole_spec(out_kernel.shape)],
        out_shape=[struct(join_kernel.shape, F32), struct(out_kernel.shape, F32)],
    )(total)
    recon = jnp.concatenate([ce[:, :1], cm, ce[:, 1:]], 1).transpose(0, 2, 1, 3)
    return recon, join_total, out_total


def solution(mesh):
    placed = (
        P(("parts", "frame"), None, "tile", None),
        P(("parts", "frame"), None, "tile", None),
        P("parts", None),
        P("parts"),
        P("parts"),
        P("parts"),
        P(),
        P(),
    )
    return jax.shard_map(
        on_device,
        mesh=mesh,
        in_specs=placed,
        out_specs=(
            P(("parts", "frame"), None, "tile", None),
            P("parts", None, None, None),
            P("parts", None, None, None),
        ),
        check_vma=False,
    )
```

```python
import functools

import jax
import jax.numpy as jnp
from jax import lax
from jax.experimental.layout import Layout, with_layout_constraint
from jax.experimental import pallas as pl
from jax.experimental.pallas import tpu as pltpu
from jax.sharding import PartitionSpec as P

F32 = jnp.float32
BF16 = jnp.bfloat16
LANES = 128
VMEM_LIMIT = 16 * 1024 * 1024


def call(body, name, flops, nbytes, vmem, **kw):
    return pl.pallas_call(
        body,
        name=name,
        cost_estimate=pl.CostEstimate(flops=flops, bytes_accessed=nbytes, transcendentals=0),
        compiler_params=pltpu.CompilerParams(vmem_limit_bytes=vmem),
        **kw,
    )


def whole_spec(shape):
    return pl.BlockSpec(shape, lambda *_: (0,) * len(shape))


def from_left(x):
    lane = lax.broadcasted_iota(jnp.int32, x.shape, 1)
    return jnp.where(lane == 0, jnp.zeros((), x.dtype), pltpu.roll(x, 1, 1))


def from_right(x):
    lane = lax.broadcasted_iota(jnp.int32, x.shape, 1)
    w = x.shape[1]
    return jnp.where(lane == w - 1, jnp.zeros((), x.dtype), pltpu.roll(x, w - 1, 1))


def shift_sum(y):
    c = y.shape[0] // 3
    return y[c : 2 * c] + from_left(y[:c]) + from_right(y[2 * c :])


def conv_rows(weights, rows, width, group=2):
    zero = jnp.zeros_like(rows[0])
    padded = [zero] + rows + [zero]
    sums = []
    for r0 in range(0, len(rows), group):
        columns = [
            jnp.concatenate(padded[r : r + 3], 0) for r in range(r0, min(r0 + group, len(rows)))
        ]
        y = jnp.dot(weights, jnp.concatenate(columns, 1), preferred_element_type=F32)
        for j in range(len(columns)):
            sums.append(shift_sum(y[:, j * width : (j + 1) * width]))
    return sums


def gather_body(pairs, slots, group, refs, out, *scratch, owner, frames):
    local_refs = refs.shape[0]
    picks = out.shape[0]
    g = group[0]
    wanted = (g if owner == 0 else 1 - g) * frames
    tiles, sems = (out, scratch[0]) if owner == 0 else scratch[:2]

    def fetch(i):
        slot = slots[pairs[i % 2, wanted + i // 2]] - g * local_refs
        slot = jnp.clip(slot, 0, local_refs - 1)
        return pltpu.make_async_copy(refs.at[slot], tiles.at[i], sems.at[i])

    def put(i):
        return pltpu.make_async_copy(tiles.at[i], out.at[i], scratch[2].at[i])

    for i in range(picks):
        fetch(i).start()
    for i in range(picks):
        fetch(i).wait()
        if owner:
            put(i).start()
    if owner:
        for i in range(picks):
            put(i).wait()


def prepare_body(jk, ok, w1, w2, w3, back):
    channels = ok.shape[1]
    taps = 3 * channels
    w1[...] = jnp.concatenate([jk[p * taps : (p + 1) * taps, :] for p in range(3)], 1)
    w2[...] = jnp.concatenate([ok[p * taps : (p + 1) * taps, :] for p in range(3)], 1)
    blocks = []
    for p in range(3):
        rows = []
        for q in range(3):
            at = ((2 - p) * 3 + 2 - q) * channels
            rows.append(ok[at : at + channels, :].astype(F32).T.astype(BF16))
        blocks.append(jnp.concatenate(rows, 0))
        back[p * taps : (p + 1) * taps, :] = blocks[-1]
    w3[...] = jnp.concatenate(blocks, 1)


def inside(tile, count, above, below):
    t = tile[0]
    return jnp.where(t > 0, above, jnp.zeros_like(above)), jnp.where(
        t < count - 1, below, jnp.zeros_like(below)
    )


def edge_sums(w, p, cells):
    taps = w.shape[0] // 3
    width = cells[0].shape[1]
    y = jnp.dot(
        w[p * taps : (p + 1) * taps, :],
        jnp.concatenate(cells, 1),
        preferred_element_type=F32,
    )
    return [shift_sum(y[:, k * width : (k + 1) * width]) for k in range(len(cells))]


def edge_taps_body(xr0, xc0, xr1, xc1, w, up, down):
    frames = up.shape[0]
    for xr, xc, p, out in ((xr0, xc0, 2, up), (xr1, xc1, 0, down)):
        cells = [jnp.concatenate([xr[b, 0], xc[b, 0]], 0) for b in range(frames)]
        for b, x in enumerate(edge_sums(w, p, cells)):
            out[b] = x.astype(BF16)


def silu_and_slope(v):
    s = jax.nn.sigmoid(v)
    return (v * s).astype(BF16), s * (1.0 + v * (1.0 - s))


def join_body(xr, xc, w, hidden, slope, top, bottom):
    rows, width = xr.shape[1], xr.shape[3]
    stacked = [jnp.concatenate([xr[0, r], xc[0, r]], 0) for r in range(rows)]
    sums = conv_rows(w[...], stacked, width)
    top[0] = sums[0]
    bottom[0] = sums[-1]
    for r in range(1, rows - 1):
        hidden[0, r - 1], slope[0, r - 1] = silu_and_slope(sums[r])


def join_edge_body(tile, top, bottom, above, below, ht, hb, st, sb, *, count):
    for b in range(top.shape[0]):
        got_a, got_b = inside(tile, count, above[b].astype(F32), below[b].astype(F32))
        ht[b], st[b] = silu_and_slope(top[b] + got_a)
        hb[b], sb[b] = silu_and_slope(bottom[b] + got_b)


def frame_scale(numbers, rates, group, cells, b, frames):
    return rates[numbers[group[0] * frames + b]] * (2.0 / cells)


def column(first, mid, last):
    return [first[0]] + [mid[0, r] for r in range(mid.shape[1])] + [last[0]]


def output_body(
    numbers, rates, group, hm, ht, hb, xc, w, recon, residual, top, bottom, *, cells, frames
):
    hidden = column(ht, hm, hb)
    sums = conv_rows(w[...], hidden, hm.shape[3])
    scale = frame_scale(numbers, rates, group, cells, pl.program_id(0), frames)
    top[0] = sums[0]
    bottom[0] = sums[-1]
    for r in range(1, len(sums) - 1):
        recon[0, r - 1] = sums[r].astype(BF16)
        residual[0, r - 1] = ((sums[r] - xc[0, r].astype(F32)) * scale).astype(BF16)


def output_edge_body(
    numbers, rates, group, tile, top, bottom, above, below, xc0, xc1, w, ct, cb, rt, rb,
    *, cells, frames, count
):
    frames = top.shape[0]
    got = inside(tile, count, above[...], below[...])
    for g, p, part, xc, c, r in (
        (got[0], 0, top, xc0, ct, rt),
        (got[1], 2, bottom, xc1, cb, rb),
    ):
        for b, x in enumerate(edge_sums(w, p, [g[b] for b in range(frames)])):
            scale = frame_scale(numbers, rates, group, cells, b, frames)
            total = part[b] + x
            c[b] = total.astype(BF16)
            r[b] = ((total - xc[b, 0].astype(F32)) * scale).astype(BF16)


def slope_body(rm, rt, rb, slope, w, grad, top, bottom):
    sums = conv_rows(w[...], column(rt, rm, rb), rm.shape[3])
    top[0] = sums[0]
    bottom[0] = sums[-1]
    for r in range(1, len(sums) - 1):
        grad[0, r - 1] = (sums[r] * slope[0, r - 1]).astype(BF16)


def slope_edge_body(tile, top, bottom, above, below, st, sb, w, gt, gb, *, count):
    got = inside(tile, count, above[...], below[...])
    for g, p, part, slope, grad in ((got[0], 0, top, st, gt), (got[1], 2, bottom, sb, gb)):
        for b, x in enumerate(edge_sums(w, p, [g[b] for b in range(g.shape[0])])):
            grad[b] = ((part[b] + x) * slope[b]).astype(BF16)


def contract(left, right):
    return lax.dot_general(left, right, (((1,), (1,)), ((), ())), preferred_element_type=F32)


def lane_blocks(x):
    return [x[:, k : k + LANES] for k in range(0, x.shape[1], LANES)]


def add_up(out, value):
    first = pl.program_id(0) == 0

    @pl.when(first)
    def _():
        out[...] = value

    @pl.when(jnp.logical_not(first))
    def _():
        out[...] += value


def side_taps(rows):
    return [[from_left(x) for x in rows], rows, [from_right(x) for x in rows]]


def out_grad_body(hm, ht, hb, rm, rt, rb, out):
    hidden = side_taps(column(ht, hm, hb))
    residual = column(rt, rm, rb)
    zero = jnp.zeros_like(residual[0])
    padded = [zero] + residual + [zero]
    rows = len(residual)
    value = contract(
        jnp.concatenate(
            [jnp.concatenate(padded[2 - p : 2 - p + rows], 1) for p in range(3)], 0
        ),
        jnp.concatenate([jnp.concatenate(h, 1) for h in hidden], 0),
    )
    add_up(out, value)


def grads_body(tile, gm, gt, gb, xr, xc, ht, hb, above, below, og, packed, *, count):
    rows, width = xr.shape[1], xr.shape[3]
    channels = gm.shape[2]
    joined = xr.shape[2] + xc.shape[2]
    rest = joined % 256
    head = joined - rest
    zero = jnp.zeros((channels, width), BF16)
    turned = side_taps(column(gt, gm, gb))[::-1]
    stacked = [jnp.concatenate([xr[0, r], xc[0, r]], 0) for r in range(rows)]
    taps = []
    for p in range(3):
        for q in range(3):
            taps.append(
                jnp.concatenate(
                    [turned[q][r - p + 1] if 0 <= r - p + 1 < rows else zero for r in range(rows)],
                    1,
                )
            )
    main = contract(jnp.concatenate(taps, 0), jnp.concatenate([s[:head] for s in stacked], 1))
    tails = [s[head:] for s in stacked]
    tail_zero = jnp.zeros_like(tails[0])
    tail = contract(
        jnp.concatenate([jnp.concatenate(turned[q], 1) for q in range(3)], 0),
        jnp.concatenate(
            [
                jnp.concatenate(
                    [tails[r + p - 1] if 0 <= r + p - 1 < rows else tail_zero for r in range(rows)],
                    1,
                )
                for p in range(3)
            ],
            0,
        ),
    )
    got = inside(tile, count, above[0], below[0])
    out = jnp.concatenate(
        [
            contract(got[1], jnp.concatenate([x[0] for x in side_taps([hb[0]])], 0)),
            jnp.zeros((channels, 3 * channels), F32),
            contract(got[0], jnp.concatenate([x[0] for x in side_taps([ht[0]])], 0)),
        ],
        0,
    )
    first = pl.program_id(0) == 0
    out = out + jnp.where(first, og[...], 0.0)
    blocks = lane_blocks(main) + lane_blocks(jnp.concatenate([out, tail], 1))

    @pl.when(first)
    def _():
        at = 0
        for block in blocks:
            packed[at : at + block.shape[0], :] = block
            at += block.shape[0]
        if at < packed.shape[0]:
            packed[at:, :] = jnp.zeros((packed.shape[0] - at, LANES), F32)

    @pl.when(jnp.logical_not(first))
    def _():
        at = 0
        for block in blocks:
            packed[at : at + block.shape[0], :] += block
            at += block.shape[0]


def grads_edge_body(
    tile, group, packed_in, above, below, xr0, xc0, xr1, xc1, send, keep, packed, *, count
):
    frames, channels, _ = above.shape
    joined = xr0.shape[2] + xc0.shape[2]
    rest = joined % 256
    head = joined - rest
    taps = 3 * channels
    half = send.shape[0]
    packed[...] = packed_in[...]
    tail_at = 3 * taps * (head // LANES)
    got = inside(tile, count, above[...], below[...])
    for p, edge, xr, xc in ((2, got[0], xr0, xc0), (0, got[1], xr1, xc1)):
        rows = [edge[b] for b in range(frames)]
        left = jnp.concatenate(
            [
                jnp.concatenate([move(g) for g in rows], 1)
                for move in (from_right, lambda g: g, from_left)
            ],
            0,
        )
        right = jnp.concatenate(
            [jnp.concatenate([xr[b, 0], xc[b, 0]], 0) for b in range(frames)], 1
        )
        extra = contract(left, right)
        for k, block in enumerate(lane_blocks(extra[:, :head])):
            at = 3 * taps * k + taps * p
            packed[at : at + taps, :] += block
        lane = taps + rest * p
        at = tail_at + taps * (lane // LANES)
        lane = lane % LANES
        packed[at : at + taps, lane : lane + rest] += extra[:, head:]
    g = group[0]
    send[...] = packed[pl.ds(pl.multiple_of((1 - g) * half, 8), half), :]
    keep[...] = packed[pl.ds(pl.multiple_of(g * half, 8), half), :]


def unpack_body(group, own, got, join, out, packed):
    channels = out.shape[2]
    joined = join.shape[3]
    rest = joined % 256
    head = joined - rest
    taps = 3 * channels
    half = own.shape[0]
    g = group[0]
    packed[pl.ds(pl.multiple_of(g * half, 8), half), :] = own[...].astype(F32)
    packed[pl.ds(pl.multiple_of((1 - g) * half, 8), half), :] = got[...].astype(F32)
    tail_at = 3 * taps * (head // LANES)
    tail = jnp.concatenate(
        [
            packed[tail_at + taps * k : tail_at + taps * (k + 1), :]
            for k in range((taps + 3 * rest) // LANES)
        ],
        1,
    )
    for p in range(3):
        for q in range(3):
            rows = slice(q * channels, (q + 1) * channels)
            at = taps * p + q * channels
            pieces = [
                packed[3 * taps * k + at : 3 * taps * k + at + channels, :]
                for k in range(head // LANES)
            ]
            pieces.append(tail[rows, taps + rest * p : taps + rest * (p + 1)])
            join[p, q] = jnp.concatenate(pieces, 1)
            out[p, q] = tail[p * channels : (p + 1) * channels, q * channels : (q + 1) * channels]


def swap_edges(up, down, axis):
    count = lax.axis_size(axis)
    below = lax.ppermute(up, axis, [((i + 1) % count, i) for i in range(count)])
    above = lax.ppermute(down, axis, [(i, (i + 1) % count) for i in range(count)])
    return above, below


def halves(part, axis, stride):
    bit = (lax.axis_index(axis) // stride) % 2
    half = part.shape[0] // 2
    send = lax.dynamic_slice_in_dim(part, (1 - bit) * half, half, 0)
    return send, lax.dynamic_slice_in_dim(part, bit * half, half, 0)


def on_device(
    decoded_refs,
    current_frames,
    ref_pairs,
    ref_slots,
    frame_numbers,
    rate_weights,
    join_kernel,
    out_kernel,
):
    local_refs = decoded_refs.shape[0]
    frames, channels, rows, width = current_frames.shape
    joined = join_kernel.shape[3]
    count = lax.axis_size("tile")
    cells = rows * count * width
    group = lax.axis_index("frame")
    group_id = group.reshape(1).astype(jnp.int32)
    tile_id = lax.axis_index("tile").reshape(1).astype(jnp.int32)
    picks = 2 * frames
    taps = 3 * channels
    conv_flops = 2 * frames * rows * width * 3 * taps

    def struct(shape, dtype):
        return jax.ShapeDtypeStruct(shape, dtype)

    def run(
        body, name, scalars, args, specs, outs, out_specs, grid, flops, nbytes, scratch=(),
        vmem=VMEM_LIMIT,
    ):
        return call(
            body,
            name,
            flops,
            nbytes,
            vmem,
            grid_spec=pltpu.PrefetchScalarGridSpec(
                num_scalar_prefetch=len(scalars),
                grid=grid,
                in_specs=specs,
                out_specs=out_specs,
                scratch_shapes=scratch,
            ),
            out_shape=outs,
        )(*scalars, *args)

    def each(x):
        return pl.BlockSpec((1,) + x.shape[1:], lambda b, *_: (b,) + (0,) * (len(x.shape) - 1))

    def whole(x):
        return whole_spec(x.shape)

    def row(x, r):
        return pl.BlockSpec((frames, 1) + x.shape[2:], lambda *_: (0, r, 0, 0))

    pairs_of = ref_pairs.T
    tile_shape = decoded_refs.shape[1:]

    def gathered(owner, name):
        return run(
            functools.partial(gather_body, owner=owner, frames=frames),
            name,
            (pairs_of, ref_slots, group_id),
            (pltpu.with_memory_space_constraint(decoded_refs, pltpu.HBM),),
            [pl.BlockSpec(memory_space=pltpu.HBM)],
            struct((picks,) + tile_shape, BF16),
            pl.BlockSpec(memory_space=pltpu.HBM if owner else pltpu.VMEM),
            (1,),
            0,
            4 * picks * channels * rows * width,
            ((pltpu.VMEM((picks,) + tile_shape, BF16),) if owner else ())
            + (pltpu.SemaphoreType.DMA((picks,)),) * (1 + owner),
            60 * 1024 * 1024 if owner else VMEM_LIMIT,
        )

    incoming = lax.ppermute(gathered(1, "gather_out"), "frame", [(0, 1), (1, 0)])
    own = gathered(0, "gather_own")
    pairs = lax.dynamic_slice_in_dim(ref_pairs, group * frames, frames, 0)
    slot_range = jnp.arange(ref_slots.shape[0], dtype=jnp.int32)
    slots = jnp.sum(jnp.where(pairs[:, :, None] == slot_range, ref_slots, 0), axis=-1)
    held = slots // local_refs == group
    picked = jnp.where(
        held[:, :, None, None, None],
        own.reshape(frames, 2, channels, rows, width),
        incoming.reshape(frames, 2, channels, rows, width),
    )
    xr = picked.transpose(0, 3, 1, 2, 4).reshape(frames, rows, 2 * channels, width)
    xc = current_frames.transpose(0, 2, 1, 3)

    jk = join_kernel.reshape(3 * taps, joined)
    ok = out_kernel.reshape(3 * taps, channels)
    prepared = [
        struct((taps, 3 * joined), BF16),
        struct((taps, taps), BF16),
        struct((taps, taps), BF16),
        struct((3 * taps, channels), BF16),
    ]
    w1, w2, w3, back = run(
        prepare_body, "prepare", (), (jk, ok), [whole(jk), whole(ok)], prepared,
        [whole(x) for x in prepared], (1,), 4 * jk.size, 4 * (jk.size + 3 * ok.size),
    )

    mid = (frames, rows - 2, channels, width)
    line = (frames, channels, width)
    mid_b, mid_f = struct(mid, BF16), struct(mid, F32)
    line_b, line_f = struct(line, BF16), struct(line, F32)
    edge_bytes = 24 * frames * channels * width
    mid_bytes = 10 * frames * rows * channels * width
    edge_flops = conv_flops * channels // (3 * rows) * 2

    up, down = run(
        edge_taps_body, "edge_taps", (), (xr, xc, xr, xc, jk),
        [row(xr, 0), row(xc, 0), row(xr, rows - 1), row(xc, rows - 1), whole(jk)],
        [line_b] * 2, [whole(line_b)] * 2, (1,), 3 * edge_flops, edge_bytes,
    )
    above, below = swap_edges(up, down, "tile")

    outs = [mid_b, mid_f, line_f, line_f]
    hm, sm, top, bottom = run(
        join_body, "join_conv", (), (xr, xc, w1), [each(xr), each(xc), whole(w1)],
        outs, [each(x) for x in outs], (frames,), conv_flops * joined, mid_bytes,
    )
    ht, hb, st, sb = run(
        functools.partial(join_edge_body, count=count), "join_edge", (tile_id,),
        (top, bottom, above, below), [whole(line_f)] * 4,
        [line_b, line_b, line_f, line_f], [whole(line_f)] * 4, (1,), edge_bytes, edge_bytes,
    )
    h_above, h_below = swap_edges(ht, hb, "tile")

    rated = (frame_numbers, rate_weights, group_id)
    outs = [mid_b, mid_b, line_f, line_f]
    cm, rm, top, bottom = run(
        functools.partial(output_body, cells=cells, frames=frames), "out_conv", rated,
        (hm, ht, hb, xc, w2), [each(x) for x in (hm, ht, hb, xc)] + [whole(w2)],
        outs, [each(x) for x in outs], (frames,), conv_flops * channels, mid_bytes,
    )
    ct, cb, rt, rb = run(
        functools.partial(output_edge_body, cells=cells, frames=frames, count=count),
        "out_edge", rated + (tile_id,), (top, bottom, h_above, h_below, xc, xc, ok),
        [whole(line_f)] * 4 + [row(xc, 0), row(xc, rows - 1), whole(ok)],
        [line_b] * 4, [whole(line_b)] * 4, (1,), edge_flops, edge_bytes,
    )
    r_above, r_below = swap_edges(rt, rb, "tile")

    outs = [mid_b, line_f, line_f]
    gm, top, bottom = run(
        slope_body, "back_conv", (), (rm, rt, rb, sm, w3),
        [each(x) for x in (rm, rt, rb, sm)] + [whole(w3)],
        outs, [each(x) for x in outs], (frames,), conv_flops * channels, mid_bytes,
    )
    og_s = struct((taps, taps), F32)
    og = run(
        out_grad_body, "out_grad", (), (hm, ht, hb, rm, rt, rb),
        [each(x) for x in (hm, ht, hb, rm, rt, rb)], og_s, whole(og_s), (frames,),
        conv_flops * channels, mid_bytes,
    )
    recon = jnp.concatenate([ct[:, None], cm, cb[:, None]], 1).transpose(0, 2, 1, 3)
    recon = with_layout_constraint(recon, Layout((0, 1, 2, 3)))
    gt, gb = run(
        functools.partial(slope_edge_body, count=count), "back_edge", (tile_id,),
        (top, bottom, r_above, r_below, st, sb, back), [whole(line_f)] * 6 + [whole(back)],
        [line_b] * 2, [whole(line_b)] * 2, (1,), edge_flops, edge_bytes,
    )
    g_above, g_below = swap_edges(gt, gb, "tile")

    strides = []
    while 1 << len(strides) < count:
        strides.append(1 << len(strides))
    unit = 8 * 2 * count
    packed_rows = 3 * taps * (joined + channels) // LANES
    packed_s = struct((pl.cdiv(packed_rows, unit) * unit, LANES), F32)
    half_s = struct((packed_s.shape[0] // 2, LANES), F32)
    args = (gm, gt, gb, xr, xc, ht, hb, r_above, r_below)
    packed = run(
        functools.partial(grads_body, count=count), "grads", (tile_id,), args + (og,),
        [each(x) for x in args] + [whole(og)], packed_s, whole(packed_s), (frames,),
        conv_flops * joined, 2 * mid_bytes,
    )
    send, part = run(
        functools.partial(grads_edge_body, count=count), "grads_edge", (tile_id, group_id),
        (packed, g_above, g_below, xr, xc, xr, xc),
        [whole(packed_s), whole(line_b), whole(line_b)]
        + [row(xr, 0), row(xc, 0), row(xr, rows - 1), row(xc, rows - 1)],
        [half_s] * 2, [whole(half_s)] * 2, (1,), 3 * edge_flops, edge_bytes,
        (pltpu.VMEM(packed_s.shape, F32),),
    )
    part = part + lax.ppermute(send, "frame", [(0, 1), (1, 0)])
    for stride in strides[:-1]:
        send, keep = halves(part, "tile", stride)
        pairs = [(i, i ^ stride) for i in range(count)]
        part = keep + lax.ppermute(send.astype(BF16), "tile", pairs).astype(F32)
    part = part.astype(BF16)
    pairs = [(i, i ^ strides[-1]) for i in range(count)]
    got = lax.ppermute(part, "tile", pairs)
    part = (part.astype(F32) + got.astype(F32)).astype(BF16)
    part, recon = lax.optimization_barrier((part, recon))
    for stride in reversed(strides[:-1]):
        bit = (lax.axis_index("tile") // stride) % 2
        got = lax.ppermute(part, "tile", [(i, i ^ stride) for i in range(count)])
        part = jnp.concatenate(
            [jnp.where(bit == 0, part, got), jnp.where(bit == 0, got, part)], 0
        )
    got = lax.ppermute(part, "frame", [(0, 1), (1, 0)])
    outs = [struct(join_kernel.shape, F32), struct(out_kernel.shape, F32)]
    join_total, out_total = run(
        unpack_body, "unpack", (group_id,), (part, got), [whole(half_s)] * 2,
        outs, [whole(x) for x in outs], (1,), 0, 8 * packed_s.size,
        (pltpu.VMEM(packed_s.shape, F32),),
    )
    return recon, join_total, out_total


def solution(mesh):
    placed = (
        P(("parts", "frame"), None, "tile", None),
        P(("parts", "frame"), None, "tile", None),
        P("parts", None),
        P("parts"),
        P("parts"),
        P("parts"),
        P(),
        P(),
    )
    return jax.shard_map(
        on_device,
        mesh=mesh,
        in_specs=placed,
        out_specs=(
            P(("parts", "frame"), None, "tile", None),
            P("parts", None, None, None),
            P("parts", None, None, None),
        ),
        check_vma=False,
    )
```

```python
import functools

import jax
import jax.numpy as jnp
from jax import lax
from jax.experimental.layout import Layout, with_layout_constraint
from jax.experimental import pallas as pl
from jax.experimental.pallas import tpu as pltpu
from jax.sharding import PartitionSpec as P

F32 = jnp.float32
BF16 = jnp.bfloat16
LANES = 128
VMEM_LIMIT = 16 * 1024 * 1024


def call(body, name, flops, nbytes, vmem, **kw):
    return pl.pallas_call(
        body,
        name=name,
        cost_estimate=pl.CostEstimate(flops=flops, bytes_accessed=nbytes, transcendentals=0),
        compiler_params=pltpu.CompilerParams(vmem_limit_bytes=vmem),
        **kw,
    )


def whole_spec(shape):
    return pl.BlockSpec(shape, lambda *_: (0,) * len(shape))


def from_left(x):
    lane = lax.broadcasted_iota(jnp.int32, x.shape, 1)
    return jnp.where(lane == 0, jnp.zeros((), x.dtype), pltpu.roll(x, 1, 1))


def from_right(x):
    lane = lax.broadcasted_iota(jnp.int32, x.shape, 1)
    w = x.shape[1]
    return jnp.where(lane == w - 1, jnp.zeros((), x.dtype), pltpu.roll(x, w - 1, 1))


def shift_sum(y):
    c = y.shape[0] // 3
    return y[c : 2 * c] + from_left(y[:c]) + from_right(y[2 * c :])


def conv_rows(weights, rows, width, group=2):
    zero = jnp.zeros_like(rows[0])
    padded = [zero] + rows + [zero]
    sums = []
    for r0 in range(0, len(rows), group):
        columns = [
            jnp.concatenate(padded[r : r + 3], 0) for r in range(r0, min(r0 + group, len(rows)))
        ]
        y = jnp.dot(weights, jnp.concatenate(columns, 1), preferred_element_type=F32)
        for j in range(len(columns)):
            sums.append(shift_sum(y[:, j * width : (j + 1) * width]))
    return sums


def gather_body(pairs, slots, group, refs, out, *scratch, owner, frames):
    local_refs = refs.shape[0]
    picks = out.shape[0]
    g = group[0]
    wanted = (g if owner == 0 else 1 - g) * frames
    tiles, sems = (out, scratch[0]) if owner == 0 else scratch[:2]

    def fetch(i):
        slot = slots[pairs[i % 2, wanted + i // 2]] - g * local_refs
        slot = jnp.clip(slot, 0, local_refs - 1)
        return pltpu.make_async_copy(refs.at[slot], tiles.at[i], sems.at[i])

    def put(i):
        return pltpu.make_async_copy(tiles.at[i], out.at[i], scratch[2].at[i])

    for i in range(picks):
        fetch(i).start()
    for i in range(picks):
        fetch(i).wait()
        if owner:
            put(i).start()
    if owner:
        for i in range(picks):
            put(i).wait()


def prepare_body(jk, ok, w1, w2, w3, back):
    channels = ok.shape[1]
    taps = 3 * channels
    w1[...] = jnp.concatenate([jk[p * taps : (p + 1) * taps, :] for p in range(3)], 1)
    w2[...] = jnp.concatenate([ok[p * taps : (p + 1) * taps, :] for p in range(3)], 1)
    blocks = []
    for p in range(3):
        rows = []
        for q in range(3):
            at = ((2 - p) * 3 + 2 - q) * channels
            rows.append(ok[at : at + channels, :].astype(F32).T.astype(BF16))
        blocks.append(jnp.concatenate(rows, 0))
        back[p * taps : (p + 1) * taps, :] = blocks[-1]
    w3[...] = jnp.concatenate(blocks, 1)


def inside(tile, count, above, below):
    t = tile[0]
    return jnp.where(t > 0, above, jnp.zeros_like(above)), jnp.where(
        t < count - 1, below, jnp.zeros_like(below)
    )


def edge_sums(w, p, cells):
    taps = w.shape[0] // 3
    width = cells[0].shape[1]
    y = jnp.dot(
        w[p * taps : (p + 1) * taps, :],
        jnp.concatenate(cells, 1),
        preferred_element_type=F32,
    )
    return [shift_sum(y[:, k * width : (k + 1) * width]) for k in range(len(cells))]


def edge_taps_body(xr0, xc0, xr1, xc1, w, up, down):
    frames = up.shape[0]
    for xr, xc, p, out in ((xr0, xc0, 2, up), (xr1, xc1, 0, down)):
        cells = [jnp.concatenate([xr[b, 0], xc[b, 0]], 0) for b in range(frames)]
        for b, x in enumerate(edge_sums(w, p, cells)):
            out[b] = x.astype(BF16)


def silu_and_slope(v):
    s = jax.nn.sigmoid(v)
    return (v * s).astype(BF16), s * (1.0 + v * (1.0 - s))


def join_body(xr, xc, w, hidden, slope, top, bottom):
    rows, width = xr.shape[1], xr.shape[3]
    stacked = [jnp.concatenate([xr[0, r], xc[0, r]], 0) for r in range(rows)]
    sums = conv_rows(w[...], stacked, width)
    top[0] = sums[0]
    bottom[0] = sums[-1]
    for r in range(1, rows - 1):
        hidden[0, r - 1], slope[0, r - 1] = silu_and_slope(sums[r])


def join_edge_body(tile, top, bottom, below, above, ht, hb, st, sb, *, count):
    for b in range(top.shape[0]):
        got_a, got_b = inside(tile, count, above[b].astype(F32), below[b].astype(F32))
        ht[b], st[b] = silu_and_slope(top[b] + got_a)
        hb[b], sb[b] = silu_and_slope(bottom[b] + got_b)


def frame_scale(numbers, rates, group, cells, b, frames):
    return rates[numbers[group[0] * frames + b]] * (2.0 / cells)


def column(first, mid, last):
    return [first[0]] + [mid[0, r] for r in range(mid.shape[1])] + [last[0]]


def output_body(
    numbers, rates, group, hm, ht, hb, xc, w, recon, residual, top, bottom, *, cells, frames
):
    hidden = column(ht, hm, hb)
    sums = conv_rows(w[...], hidden, hm.shape[3])
    scale = frame_scale(numbers, rates, group, cells, pl.program_id(0), frames)
    top[0] = sums[0]
    bottom[0] = sums[-1]
    for r in range(1, len(sums) - 1):
        recon[0, r - 1] = sums[r].astype(BF16)
        residual[0, r - 1] = ((sums[r] - xc[0, r].astype(F32)) * scale).astype(BF16)


def output_edge_body(
    numbers, rates, group, tile, top, bottom, above, below, xc0, xc1, w, ct, cb, rt, rb,
    *, cells, frames, count
):
    frames = top.shape[0]
    got = inside(tile, count, above[...], below[...])
    for g, p, part, xc, c, r in (
        (got[0], 0, top, xc0, ct, rt),
        (got[1], 2, bottom, xc1, cb, rb),
    ):
        for b, x in enumerate(edge_sums(w, p, [g[b] for b in range(frames)])):
            scale = frame_scale(numbers, rates, group, cells, b, frames)
            total = part[b] + x
            c[b] = total.astype(BF16)
            r[b] = ((total - xc[b, 0].astype(F32)) * scale).astype(BF16)


def slope_body(rm, rt, rb, slope, w, grad, top, bottom):
    sums = conv_rows(w[...], column(rt, rm, rb), rm.shape[3])
    top[0] = sums[0]
    bottom[0] = sums[-1]
    for r in range(1, len(sums) - 1):
        grad[0, r - 1] = (sums[r] * slope[0, r - 1]).astype(BF16)


def slope_edge_body(tile, top, bottom, above, below, st, sb, w, gt, gb, *, count):
    got = inside(tile, count, above[...], below[...])
    for g, p, part, slope, grad in ((got[0], 0, top, st, gt), (got[1], 2, bottom, sb, gb)):
        for b, x in enumerate(edge_sums(w, p, [g[b] for b in range(g.shape[0])])):
            grad[b] = ((part[b] + x) * slope[b]).astype(BF16)


def contract(left, right):
    return lax.dot_general(left, right, (((1,), (1,)), ((), ())), preferred_element_type=F32)


def lane_blocks(x):
    return [x[:, k : k + LANES] for k in range(0, x.shape[1], LANES)]


def add_up(out, value):
    first = pl.program_id(0) == 0

    @pl.when(first)
    def _():
        out[...] = value

    @pl.when(jnp.logical_not(first))
    def _():
        out[...] += value


def side_taps(rows):
    return [[from_left(x) for x in rows], rows, [from_right(x) for x in rows]]


def out_grad_body(hm, ht, hb, rm, rt, rb, out):
    hidden = side_taps(column(ht, hm, hb))
    residual = column(rt, rm, rb)
    zero = jnp.zeros_like(residual[0])
    padded = [zero] + residual + [zero]
    rows = len(residual)
    value = contract(
        jnp.concatenate(
            [jnp.concatenate(padded[2 - p : 2 - p + rows], 1) for p in range(3)], 0
        ),
        jnp.concatenate([jnp.concatenate(h, 1) for h in hidden], 0),
    )
    add_up(out, value)


def grads_body(tile, gm, gt, gb, xr, xc, ht, hb, above, below, og, packed, *, count):
    rows, width = xr.shape[1], xr.shape[3]
    channels = gm.shape[2]
    joined = xr.shape[2] + xc.shape[2]
    rest = joined % 256
    head = joined - rest
    zero = jnp.zeros((channels, width), BF16)
    turned = side_taps(column(gt, gm, gb))[::-1]
    stacked = [jnp.concatenate([xr[0, r], xc[0, r]], 0) for r in range(rows)]
    taps = []
    for p in range(3):
        for q in range(3):
            taps.append(
                jnp.concatenate(
                    [turned[q][r - p + 1] if 0 <= r - p + 1 < rows else zero for r in range(rows)],
                    1,
                )
            )
    main = contract(jnp.concatenate(taps, 0), jnp.concatenate([s[:head] for s in stacked], 1))
    tails = [s[head:] for s in stacked]
    tail_zero = jnp.zeros_like(tails[0])
    tail = contract(
        jnp.concatenate([jnp.concatenate(turned[q], 1) for q in range(3)], 0),
        jnp.concatenate(
            [
                jnp.concatenate(
                    [tails[r + p - 1] if 0 <= r + p - 1 < rows else tail_zero for r in range(rows)],
                    1,
                )
                for p in range(3)
            ],
            0,
        ),
    )
    got = inside(tile, count, above[0], below[0])
    out = jnp.concatenate(
        [
            contract(got[1], jnp.concatenate([x[0] for x in side_taps([hb[0]])], 0)),
            jnp.zeros((channels, 3 * channels), F32),
            contract(got[0], jnp.concatenate([x[0] for x in side_taps([ht[0]])], 0)),
        ],
        0,
    )
    first = pl.program_id(0) == 0
    out = out + jnp.where(first, og[...], 0.0)
    blocks = lane_blocks(main) + lane_blocks(jnp.concatenate([out, tail], 1))

    @pl.when(first)
    def _():
        at = 0
        for block in blocks:
            packed[at : at + block.shape[0], :] = block
            at += block.shape[0]
        if at < packed.shape[0]:
            packed[at:, :] = jnp.zeros((packed.shape[0] - at, LANES), F32)

    @pl.when(jnp.logical_not(first))
    def _():
        at = 0
        for block in blocks:
            packed[at : at + block.shape[0], :] += block
            at += block.shape[0]


def grads_edge_body(
    tile, group, packed_in, above, below, xr0, xc0, xr1, xc1, send, keep, packed, *, count
):
    frames, channels, _ = above.shape
    joined = xr0.shape[2] + xc0.shape[2]
    rest = joined % 256
    head = joined - rest
    taps = 3 * channels
    half = send.shape[0]
    packed[...] = packed_in[...]
    tail_at = 3 * taps * (head // LANES)
    got = inside(tile, count, above[...], below[...])
    for p, edge, xr, xc in ((2, got[0], xr0, xc0), (0, got[1], xr1, xc1)):
        rows = [edge[b] for b in range(frames)]
        left = jnp.concatenate(
            [
                jnp.concatenate([move(g) for g in rows], 1)
                for move in (from_right, lambda g: g, from_left)
            ],
            0,
        )
        right = jnp.concatenate(
            [jnp.concatenate([xr[b, 0], xc[b, 0]], 0) for b in range(frames)], 1
        )
        extra = contract(left, right)
        for k, block in enumerate(lane_blocks(extra[:, :head])):
            at = 3 * taps * k + taps * p
            packed[at : at + taps, :] += block
        lane = taps + rest * p
        at = tail_at + taps * (lane // LANES)
        lane = lane % LANES
        packed[at : at + taps, lane : lane + rest] += extra[:, head:]
    g = group[0]
    send[...] = packed[pl.ds(pl.multiple_of((1 - g) * half, 8), half), :].astype(BF16)
    keep[...] = packed[pl.ds(pl.multiple_of(g * half, 8), half), :]


def unpack_body(group, tile, own, got, join, out, packed, *, near):
    channels = out.shape[2]
    joined = join.shape[3]
    rest = joined % 256
    head = joined - rest
    taps = 3 * channels
    half = own.shape[0]
    g = group[0]
    size = half // near
    me = lax.rem(tile[0], near)
    for k in range(near):
        at = (me ^ k) * size
        for held, x in ((g, own), (1 - g, got)):
            packed[pl.ds(pl.multiple_of(held * half + at, 8), size), :] = x[
                k * size : (k + 1) * size, :
            ].astype(F32)
    tail_at = 3 * taps * (head // LANES)
    tail = jnp.concatenate(
        [
            packed[tail_at + taps * k : tail_at + taps * (k + 1), :]
            for k in range((taps + 3 * rest) // LANES)
        ],
        1,
    )
    for p in range(3):
        for q in range(3):
            rows = slice(q * channels, (q + 1) * channels)
            at = taps * p + q * channels
            pieces = [
                packed[3 * taps * k + at : 3 * taps * k + at + channels, :]
                for k in range(head // LANES)
            ]
            pieces.append(tail[rows, taps + rest * p : taps + rest * (p + 1)])
            join[p, q] = jnp.concatenate(pieces, 1)
            out[p, q] = tail[p * channels : (p + 1) * channels, q * channels : (q + 1) * channels]


def swap_edges(up, down, axis):
    count = lax.axis_size(axis)
    below = lax.ppermute(up, axis, [((i + 1) % count, i) for i in range(count)])
    above = lax.ppermute(down, axis, [(i, (i + 1) % count) for i in range(count)])
    return above, below


def on_device(
    decoded_refs,
    current_frames,
    ref_pairs,
    ref_slots,
    frame_numbers,
    rate_weights,
    join_kernel,
    out_kernel,
):
    local_refs = decoded_refs.shape[0]
    frames, channels, rows, width = current_frames.shape
    joined = join_kernel.shape[3]
    count = lax.axis_size("tile")
    cells = rows * count * width
    group = lax.axis_index("frame")
    group_id = group.reshape(1).astype(jnp.int32)
    tile_id = lax.axis_index("tile").reshape(1).astype(jnp.int32)
    picks = 2 * frames
    taps = 3 * channels
    conv_flops = 2 * frames * rows * width * 3 * taps

    def struct(shape, dtype):
        return jax.ShapeDtypeStruct(shape, dtype)

    def run(
        body, name, scalars, args, specs, outs, out_specs, grid, flops, nbytes, scratch=(),
        vmem=VMEM_LIMIT,
    ):
        return call(
            body,
            name,
            flops,
            nbytes,
            vmem,
            grid_spec=pltpu.PrefetchScalarGridSpec(
                num_scalar_prefetch=len(scalars),
                grid=grid,
                in_specs=specs,
                out_specs=out_specs,
                scratch_shapes=scratch,
            ),
            out_shape=outs,
        )(*scalars, *args)

    def each(x):
        return pl.BlockSpec((1,) + x.shape[1:], lambda b, *_: (b,) + (0,) * (len(x.shape) - 1))

    def whole(x):
        return whole_spec(x.shape)

    def row(x, r):
        return pl.BlockSpec((frames, 1) + x.shape[2:], lambda *_: (0, r, 0, 0))

    pairs_of = ref_pairs.T
    tile_shape = decoded_refs.shape[1:]

    def gathered(owner, name):
        return run(
            functools.partial(gather_body, owner=owner, frames=frames),
            name,
            (pairs_of, ref_slots, group_id),
            (pltpu.with_memory_space_constraint(decoded_refs, pltpu.HBM),),
            [pl.BlockSpec(memory_space=pltpu.HBM)],
            struct((picks,) + tile_shape, BF16),
            pl.BlockSpec(memory_space=pltpu.HBM if owner else pltpu.VMEM),
            (1,),
            0,
            4 * picks * channels * rows * width,
            ((pltpu.VMEM((picks,) + tile_shape, BF16),) if owner else ())
            + (pltpu.SemaphoreType.DMA((picks,)),) * (1 + owner),
            60 * 1024 * 1024 if owner else VMEM_LIMIT,
        )

    incoming = lax.ppermute(gathered(1, "gather_out"), "frame", [(0, 1), (1, 0)])
    own = gathered(0, "gather_own")
    pairs = lax.dynamic_slice_in_dim(ref_pairs, group * frames, frames, 0)
    slot_range = jnp.arange(ref_slots.shape[0], dtype=jnp.int32)
    slots = jnp.sum(jnp.where(pairs[:, :, None] == slot_range, ref_slots, 0), axis=-1)
    held = slots // local_refs == group
    picked = jnp.where(
        held[:, :, None, None, None],
        own.reshape(frames, 2, channels, rows, width),
        incoming.reshape(frames, 2, channels, rows, width),
    )
    xr = picked.transpose(0, 3, 1, 2, 4).reshape(frames, rows, 2 * channels, width)
    xc = current_frames.transpose(0, 2, 1, 3)

    jk = join_kernel.reshape(3 * taps, joined)
    ok = out_kernel.reshape(3 * taps, channels)
    prepared = [
        struct((taps, 3 * joined), BF16),
        struct((taps, taps), BF16),
        struct((taps, taps), BF16),
        struct((3 * taps, channels), BF16),
    ]
    w1, w2, w3, back = run(
        prepare_body, "prepare", (), (jk, ok), [whole(jk), whole(ok)], prepared,
        [whole(x) for x in prepared], (1,), 4 * jk.size, 4 * (jk.size + 3 * ok.size),
    )

    mid = (frames, rows - 2, channels, width)
    line = (frames, channels, width)
    mid_b, mid_f = struct(mid, BF16), struct(mid, F32)
    line_b, line_f = struct(line, BF16), struct(line, F32)
    edge_bytes = 24 * frames * channels * width
    mid_bytes = 10 * frames * rows * channels * width
    edge_flops = conv_flops * channels // (3 * rows) * 2

    up, down = run(
        edge_taps_body, "edge_taps", (), (xr, xc, xr, xc, jk),
        [row(xr, 0), row(xc, 0), row(xr, rows - 1), row(xc, rows - 1), whole(jk)],
        [line_b] * 2, [whole(line_b)] * 2, (1,), 3 * edge_flops, edge_bytes,
    )
    above, below = swap_edges(up, down, "tile")

    outs = [mid_b, mid_f, line_f, line_f]
    hm, sm, top, bottom = run(
        join_body, "join_conv", (), (xr, xc, w1), [each(xr), each(xc), whole(w1)],
        outs, [each(x) for x in outs], (frames,), conv_flops * joined, mid_bytes,
    )
    ht, hb, st, sb = run(
        functools.partial(join_edge_body, count=count), "join_edge", (tile_id,),
        (top, bottom, below, above), [whole(line_f)] * 4,
        [line_b, line_b, line_f, line_f], [whole(line_f)] * 4, (1,), edge_bytes, edge_bytes,
    )
    h_above, h_below = swap_edges(ht, hb, "tile")

    rated = (frame_numbers, rate_weights, group_id)
    outs = [mid_b, mid_b, line_f, line_f]
    cm, rm, top, bottom = run(
        functools.partial(output_body, cells=cells, frames=frames), "out_conv", rated,
        (hm, ht, hb, xc, w2), [each(x) for x in (hm, ht, hb, xc)] + [whole(w2)],
        outs, [each(x) for x in outs], (frames,), conv_flops * channels, mid_bytes,
    )
    ct, cb, rt, rb = run(
        functools.partial(output_edge_body, cells=cells, frames=frames, count=count),
        "out_edge", rated + (tile_id,), (top, bottom, h_above, h_below, xc, xc, ok),
        [whole(line_f)] * 4 + [row(xc, 0), row(xc, rows - 1), whole(ok)],
        [line_b] * 4, [whole(line_b)] * 4, (1,), edge_flops, edge_bytes,
    )
    r_above, r_below = swap_edges(rt, rb, "tile")

    outs = [mid_b, line_f, line_f]
    gm, top, bottom = run(
        slope_body, "back_conv", (), (rm, rt, rb, sm, w3),
        [each(x) for x in (rm, rt, rb, sm)] + [whole(w3)],
        outs, [each(x) for x in outs], (frames,), conv_flops * channels, mid_bytes,
    )
    og_s = struct((taps, taps), F32)
    og = run(
        out_grad_body, "out_grad", (), (hm, ht, hb, rm, rt, rb),
        [each(x) for x in (hm, ht, hb, rm, rt, rb)], og_s, whole(og_s), (frames,),
        conv_flops * channels, mid_bytes,
    )
    recon = jnp.concatenate([ct[:, None], cm, cb[:, None]], 1).transpose(0, 2, 1, 3)
    recon = with_layout_constraint(recon, Layout((0, 1, 2, 3)))
    gt, gb = run(
        functools.partial(slope_edge_body, count=count), "back_edge", (tile_id,),
        (top, bottom, r_above, r_below, st, sb, back), [whole(line_f)] * 6 + [whole(back)],
        [line_b] * 2, [whole(line_b)] * 2, (1,), edge_flops, edge_bytes,
    )
    g_above, g_below = swap_edges(gt, gb, "tile")

    near = 4 if count % 4 == 0 else count
    unit = 16 * 2 * near
    packed_rows = 3 * taps * (joined + channels) // LANES
    packed_s = struct((pl.cdiv(packed_rows, unit) * unit, LANES), F32)
    half_s = struct((packed_s.shape[0] // 2, LANES), F32)
    args = (gm, gt, gb, xr, xc, ht, hb, r_above, r_below)
    packed = run(
        functools.partial(grads_body, count=count), "grads", (tile_id,), args + (og,),
        [each(x) for x in args] + [whole(og)], packed_s, whole(packed_s), (frames,),
        conv_flops * joined, 2 * mid_bytes,
    )
    send, part = run(
        functools.partial(grads_edge_body, count=count), "grads_edge", (tile_id, group_id),
        (packed, g_above, g_below, xr, xc, xr, xc),
        [whole(packed_s), whole(line_b), whole(line_b)]
        + [row(xr, 0), row(xc, 0), row(xr, rows - 1), row(xc, rows - 1)],
        [struct(half_s.shape, BF16), half_s], [whole(half_s)] * 2, (1,), 3 * edge_flops, edge_bytes,
        (pltpu.VMEM(packed_s.shape, F32),),
    )
    part = part + lax.ppermute(send, "frame", [(0, 1), (1, 0)]).astype(F32)
    me = lax.axis_index("tile") % near
    size = part.shape[0] // near

    def trade(x, mask):
        return lax.ppermute(x, "tile", [(i, i ^ mask) for i in range(count)])

    def quarter(mask):
        return lax.dynamic_slice_in_dim(part, (me ^ mask) * size, size, 0)

    gots = [trade(quarter(mask).astype(BF16), mask) for mask in range(1, near)]
    total = quarter(0)
    for got in gots:
        total = total + got.astype(F32)
    total = total.astype(BF16)
    mask = near
    while mask < count:
        total = (total.astype(F32) + trade(total, mask).astype(F32)).astype(BF16)
        mask *= 2
    total, recon = lax.optimization_barrier((total, recon))
    part = jnp.concatenate([total] + [trade(total, mask) for mask in range(1, near)], 0)
    got = lax.ppermute(part, "frame", [(0, 1), (1, 0)])
    outs = [struct(join_kernel.shape, F32), struct(out_kernel.shape, F32)]
    join_total, out_total = run(
        functools.partial(unpack_body, near=near), "unpack", (group_id, tile_id), (part, got), [whole(half_s)] * 2,
        outs, [whole(x) for x in outs], (1,), 0, 8 * packed_s.size,
        (pltpu.VMEM(packed_s.shape, F32),),
    )
    return recon, join_total, out_total


def solution(mesh):
    placed = (
        P(("parts", "frame"), None, "tile", None),
        P(("parts", "frame"), None, "tile", None),
        P("parts", None),
        P("parts"),
        P("parts"),
        P("parts"),
        P(),
        P(),
    )
    return jax.shard_map(
        on_device,
        mesh=mesh,
        in_specs=placed,
        out_specs=(
            P(("parts", "frame"), None, "tile", None),
            P("parts", None, None, None),
            P("parts", None, None, None),
        ),
        check_vma=False,
    )
```

```python
import functools

import jax
import jax.numpy as jnp
from jax import lax
from jax.experimental.layout import Layout, with_layout_constraint
from jax.experimental import pallas as pl
from jax.experimental.pallas import tpu as pltpu
from jax.sharding import PartitionSpec as P

F32 = jnp.float32
BF16 = jnp.bfloat16
LANES = 128
VMEM_LIMIT = 16 * 1024 * 1024


def call(body, name, flops, nbytes, vmem, **kw):
    return pl.pallas_call(
        body,
        name=name,
        cost_estimate=pl.CostEstimate(flops=flops, bytes_accessed=nbytes, transcendentals=0),
        compiler_params=pltpu.CompilerParams(vmem_limit_bytes=vmem),
        **kw,
    )


def whole_spec(shape):
    return pl.BlockSpec(shape, lambda *_: (0,) * len(shape))


def from_left(x):
    lane = lax.broadcasted_iota(jnp.int32, x.shape, 1)
    return jnp.where(lane == 0, jnp.zeros((), x.dtype), pltpu.roll(x, 1, 1))


def from_right(x):
    lane = lax.broadcasted_iota(jnp.int32, x.shape, 1)
    w = x.shape[1]
    return jnp.where(lane == w - 1, jnp.zeros((), x.dtype), pltpu.roll(x, w - 1, 1))


def shift_sum(y):
    c = y.shape[0] // 3
    return y[c : 2 * c] + from_left(y[:c]) + from_right(y[2 * c :])


def conv_rows(weights, rows, width, group=2):
    zero = jnp.zeros_like(rows[0])
    padded = [zero] + rows + [zero]
    sums = []
    for r0 in range(0, len(rows), group):
        columns = [
            jnp.concatenate(padded[r : r + 3], 0) for r in range(r0, min(r0 + group, len(rows)))
        ]
        y = jnp.dot(weights, jnp.concatenate(columns, 1), preferred_element_type=F32)
        for j in range(len(columns)):
            sums.append(shift_sum(y[:, j * width : (j + 1) * width]))
    return sums


def gather_body(pairs, slots, group, refs, out, *scratch, owner, frames):
    local_refs = refs.shape[0]
    picks = out.shape[0]
    g = group[0]
    wanted = (g if owner == 0 else 1 - g) * frames
    tiles, sems = (out, scratch[0]) if owner == 0 else scratch[:2]

    def fetch(i):
        slot = slots[pairs[i % 2, wanted + i // 2]] - g * local_refs
        slot = jnp.clip(slot, 0, local_refs - 1)
        return pltpu.make_async_copy(refs.at[slot], tiles.at[i], sems.at[i])

    def put(i):
        return pltpu.make_async_copy(tiles.at[i], out.at[i], scratch[2].at[i])

    for i in range(picks):
        fetch(i).start()
    for i in range(picks):
        fetch(i).wait()
        if owner:
            put(i).start()
    if owner:
        for i in range(picks):
            put(i).wait()


def prepare_body(jk, ok, w1, w2, w3, back):
    channels = ok.shape[1]
    taps = 3 * channels
    w1[...] = jnp.concatenate([jk[p * taps : (p + 1) * taps, :] for p in range(3)], 1)
    w2[...] = jnp.concatenate([ok[p * taps : (p + 1) * taps, :] for p in range(3)], 1)
    blocks = []
    for p in range(3):
        rows = []
        for q in range(3):
            at = ((2 - p) * 3 + 2 - q) * channels
            rows.append(ok[at : at + channels, :].astype(F32).T.astype(BF16))
        blocks.append(jnp.concatenate(rows, 0))
        back[p * taps : (p + 1) * taps, :] = blocks[-1]
    w3[...] = jnp.concatenate(blocks, 1)


def inside(tile, count, above, below):
    t = tile[0]
    return jnp.where(t > 0, above, jnp.zeros_like(above)), jnp.where(
        t < count - 1, below, jnp.zeros_like(below)
    )


def edge_sums(w, p, cells):
    taps = w.shape[0] // 3
    width = cells[0].shape[1]
    y = jnp.dot(
        w[p * taps : (p + 1) * taps, :],
        jnp.concatenate(cells, 1),
        preferred_element_type=F32,
    )
    return [shift_sum(y[:, k * width : (k + 1) * width]) for k in range(len(cells))]


def edge_taps_body(xr0, xc0, xr1, xc1, w, up, down):
    frames = up.shape[0]
    for xr, xc, p, out in ((xr0, xc0, 2, up), (xr1, xc1, 0, down)):
        cells = [jnp.concatenate([xr[b, 0], xc[b, 0]], 0) for b in range(frames)]
        for b, x in enumerate(edge_sums(w, p, cells)):
            out[b] = x.astype(BF16)


def silu_and_slope(v):
    s = jax.nn.sigmoid(v)
    return (v * s).astype(BF16), s * (1.0 + v * (1.0 - s))


def join_body(xr, xc, w, hidden, slope, top, bottom):
    rows, width = xr.shape[1], xr.shape[3]
    stacked = [jnp.concatenate([xr[0, r], xc[0, r]], 0) for r in range(rows)]
    sums = conv_rows(w[...], stacked, width)
    top[0] = sums[0]
    bottom[0] = sums[-1]
    for r in range(1, rows - 1):
        hidden[0, r - 1], slope[0, r - 1] = silu_and_slope(sums[r])


def join_edge_body(tile, top, bottom, below, above, ht, hb, st, sb, *, count):
    for b in range(top.shape[0]):
        got_a, got_b = inside(tile, count, above[b].astype(F32), below[b].astype(F32))
        ht[b], st[b] = silu_and_slope(top[b] + got_a)
        hb[b], sb[b] = silu_and_slope(bottom[b] + got_b)


def frame_scale(numbers, rates, group, cells, b, frames):
    return rates[numbers[group[0] * frames + b]] * (2.0 / cells)


def column(first, mid, last):
    return [first[0]] + [mid[0, r] for r in range(mid.shape[1])] + [last[0]]


def output_body(
    numbers, rates, group, hm, ht, hb, xc, w, recon, residual, top, bottom, scales,
    *, cells, frames
):
    hidden = column(ht, hm, hb)
    sums = conv_rows(w[...], hidden, hm.shape[3])
    scale = frame_scale(numbers, rates, group, cells, pl.program_id(0), frames)
    top[0] = sums[0]
    bottom[0] = sums[-1]
    scales[0] = jnp.full(scales.shape[1:], scale, F32)
    for r in range(1, len(sums) - 1):
        recon[0, r - 1] = sums[r].astype(BF16)
        residual[0, r - 1] = ((sums[r] - xc[0, r].astype(F32)) * scale).astype(BF16)


def output_edge_body(
    tile, top, bottom, above, below, xc0, xc1, scales, w, ct, cb, rt, rb, *, count
):
    frames = top.shape[0]
    got = inside(tile, count, above[...], below[...])
    for g, p, part, xc, c, r in (
        (got[0], 0, top, xc0, ct, rt),
        (got[1], 2, bottom, xc1, cb, rb),
    ):
        for b, x in enumerate(edge_sums(w, p, [g[b] for b in range(frames)])):
            total = part[b] + x
            c[b] = total.astype(BF16)
            r[b] = ((total - xc[b, 0].astype(F32)) * scales[b, :1, :]).astype(BF16)


def slope_body(rm, rt, rb, slope, w, grad, top, bottom):
    sums = conv_rows(w[...], column(rt, rm, rb), rm.shape[3])
    top[0] = sums[0]
    bottom[0] = sums[-1]
    for r in range(1, len(sums) - 1):
        grad[0, r - 1] = (sums[r] * slope[0, r - 1]).astype(BF16)


def slope_edge_body(tile, top, bottom, above, below, st, sb, w, gt, gb, *, count):
    got = inside(tile, count, above[...], below[...])
    for g, p, part, slope, grad in ((got[0], 0, top, st, gt), (got[1], 2, bottom, sb, gb)):
        for b, x in enumerate(edge_sums(w, p, [g[b] for b in range(g.shape[0])])):
            grad[b] = ((part[b] + x) * slope[b]).astype(BF16)


def contract(left, right):
    return lax.dot_general(left, right, (((1,), (1,)), ((), ())), preferred_element_type=F32)


def lane_blocks(x):
    return [x[:, k : k + LANES] for k in range(0, x.shape[1], LANES)]


def add_up(out, value):
    first = pl.program_id(0) == 0

    @pl.when(first)
    def _():
        out[...] = value

    @pl.when(jnp.logical_not(first))
    def _():
        out[...] += value


def side_taps(rows):
    return [[from_left(x) for x in rows], rows, [from_right(x) for x in rows]]


def out_grad_body(hm, ht, hb, rm, rt, rb, out):
    hidden = side_taps(column(ht, hm, hb))
    residual = column(rt, rm, rb)
    zero = jnp.zeros_like(residual[0])
    padded = [zero] + residual + [zero]
    rows = len(residual)
    value = contract(
        jnp.concatenate(
            [jnp.concatenate(padded[2 - p : 2 - p + rows], 1) for p in range(3)], 0
        ),
        jnp.concatenate([jnp.concatenate(h, 1) for h in hidden], 0),
    )
    add_up(out, value)


def grads_body(tile, gm, gt, gb, xr, xc, ht, hb, above, below, og, packed, *, count):
    rows, width = xr.shape[1], xr.shape[3]
    channels = gm.shape[2]
    joined = xr.shape[2] + xc.shape[2]
    rest = joined % 256
    head = joined - rest
    zero = jnp.zeros((channels, width), BF16)
    turned = side_taps(column(gt, gm, gb))[::-1]
    stacked = [jnp.concatenate([xr[0, r], xc[0, r]], 0) for r in range(rows)]
    taps = []
    for p in range(3):
        for q in range(3):
            taps.append(
                jnp.concatenate(
                    [turned[q][r - p + 1] if 0 <= r - p + 1 < rows else zero for r in range(rows)],
                    1,
                )
            )
    main = contract(jnp.concatenate(taps, 0), jnp.concatenate([s[:head] for s in stacked], 1))
    tails = [s[head:] for s in stacked]
    tail_zero = jnp.zeros_like(tails[0])
    tail = contract(
        jnp.concatenate([jnp.concatenate(turned[q], 1) for q in range(3)], 0),
        jnp.concatenate(
            [
                jnp.concatenate(
                    [tails[r + p - 1] if 0 <= r + p - 1 < rows else tail_zero for r in range(rows)],
                    1,
                )
                for p in range(3)
            ],
            0,
        ),
    )
    got = inside(tile, count, above[0], below[0])
    out = jnp.concatenate(
        [
            contract(got[1], jnp.concatenate([x[0] for x in side_taps([hb[0]])], 0)),
            jnp.zeros((channels, 3 * channels), F32),
            contract(got[0], jnp.concatenate([x[0] for x in side_taps([ht[0]])], 0)),
        ],
        0,
    )
    first = pl.program_id(0) == 0
    out = out + jnp.where(first, og[...], 0.0)
    blocks = lane_blocks(main) + lane_blocks(jnp.concatenate([out, tail], 1))

    @pl.when(first)
    def _():
        at = 0
        for block in blocks:
            packed[at : at + block.shape[0], :] = block
            at += block.shape[0]
        if at < packed.shape[0]:
            packed[at:, :] = jnp.zeros((packed.shape[0] - at, LANES), F32)

    @pl.when(jnp.logical_not(first))
    def _():
        at = 0
        for block in blocks:
            packed[at : at + block.shape[0], :] += block
            at += block.shape[0]


def grads_edge_body(
    tile, group, packed_in, above, below, xr0, xc0, xr1, xc1, send, keep, packed, *, count
):
    frames, channels, _ = above.shape
    joined = xr0.shape[2] + xc0.shape[2]
    rest = joined % 256
    head = joined - rest
    taps = 3 * channels
    half = send.shape[0]
    packed[...] = packed_in[...]
    tail_at = 3 * taps * (head // LANES)
    got = inside(tile, count, above[...], below[...])
    for p, edge, xr, xc in ((2, got[0], xr0, xc0), (0, got[1], xr1, xc1)):
        rows = [edge[b] for b in range(frames)]
        left = jnp.concatenate(
            [
                jnp.concatenate([move(g) for g in rows], 1)
                for move in (from_right, lambda g: g, from_left)
            ],
            0,
        )
        right = jnp.concatenate(
            [jnp.concatenate([xr[b, 0], xc[b, 0]], 0) for b in range(frames)], 1
        )
        extra = contract(left, right)
        for k, block in enumerate(lane_blocks(extra[:, :head])):
            at = 3 * taps * k + taps * p
            packed[at : at + taps, :] += block
        lane = taps + rest * p
        at = tail_at + taps * (lane // LANES)
        lane = lane % LANES
        packed[at : at + taps, lane : lane + rest] += extra[:, head:]
    g = group[0]
    send[...] = packed[pl.ds(pl.multiple_of((1 - g) * half, 8), half), :].astype(BF16)
    keep[...] = packed[pl.ds(pl.multiple_of(g * half, 8), half), :]


def unpack_body(group, tile, *refs, near):
    own, got, (join, out, packed) = refs[:near], refs[near : 2 * near], refs[2 * near :]
    channels = out.shape[2]
    joined = join.shape[3]
    rest = joined % 256
    head = joined - rest
    taps = 3 * channels
    size = own[0].shape[0]
    half = near * size
    g = group[0]
    me = lax.rem(tile[0], near)
    for k in range(near):
        at = (me ^ k) * size
        for held, x in ((g, own), (1 - g, got)):
            packed[pl.ds(pl.multiple_of(held * half + at, 8), size), :] = x[k][
                ...
            ].astype(F32)
    tail_at = 3 * taps * (head // LANES)
    tail = jnp.concatenate(
        [
            packed[tail_at + taps * k : tail_at + taps * (k + 1), :]
            for k in range((taps + 3 * rest) // LANES)
        ],
        1,
    )
    for p in range(3):
        for q in range(3):
            rows = slice(q * channels, (q + 1) * channels)
            at = taps * p + q * channels
            pieces = [
                packed[3 * taps * k + at : 3 * taps * k + at + channels, :]
                for k in range(head // LANES)
            ]
            pieces.append(tail[rows, taps + rest * p : taps + rest * (p + 1)])
            join[p, q] = jnp.concatenate(pieces, 1)
            out[p, q] = tail[p * channels : (p + 1) * channels, q * channels : (q + 1) * channels]


def swap_edges(up, down, axis):
    count = lax.axis_size(axis)
    below = lax.ppermute(up, axis, [((i + 1) % count, i) for i in range(count)])
    above = lax.ppermute(down, axis, [(i, (i + 1) % count) for i in range(count)])
    return above, below


def on_device(
    decoded_refs,
    current_frames,
    ref_pairs,
    ref_slots,
    frame_numbers,
    rate_weights,
    join_kernel,
    out_kernel,
):
    local_refs = decoded_refs.shape[0]
    frames, channels, rows, width = current_frames.shape
    joined = join_kernel.shape[3]
    count = lax.axis_size("tile")
    cells = rows * count * width
    group = lax.axis_index("frame")
    group_id = group.reshape(1).astype(jnp.int32)
    tile_id = lax.axis_index("tile").reshape(1).astype(jnp.int32)
    picks = 2 * frames
    taps = 3 * channels
    conv_flops = 2 * frames * rows * width * 3 * taps

    def struct(shape, dtype):
        return jax.ShapeDtypeStruct(shape, dtype)

    def run(
        body, name, scalars, args, specs, outs, out_specs, grid, flops, nbytes, scratch=(),
        vmem=VMEM_LIMIT,
    ):
        return call(
            body,
            name,
            flops,
            nbytes,
            vmem,
            grid_spec=pltpu.PrefetchScalarGridSpec(
                num_scalar_prefetch=len(scalars),
                grid=grid,
                in_specs=specs,
                out_specs=out_specs,
                scratch_shapes=scratch,
            ),
            out_shape=outs,
        )(*scalars, *args)

    def each(x):
        return pl.BlockSpec((1,) + x.shape[1:], lambda b, *_: (b,) + (0,) * (len(x.shape) - 1))

    def whole(x):
        return whole_spec(x.shape)

    def row(x, r):
        return pl.BlockSpec((frames, 1) + x.shape[2:], lambda *_: (0, r, 0, 0))

    pairs_of = ref_pairs.T
    tile_shape = decoded_refs.shape[1:]

    def gathered(owner, name):
        return run(
            functools.partial(gather_body, owner=owner, frames=frames),
            name,
            (pairs_of, ref_slots, group_id),
            (pltpu.with_memory_space_constraint(decoded_refs, pltpu.HBM),),
            [pl.BlockSpec(memory_space=pltpu.HBM)],
            struct((picks,) + tile_shape, BF16),
            pl.BlockSpec(memory_space=pltpu.HBM if owner else pltpu.VMEM),
            (1,),
            0,
            4 * picks * channels * rows * width,
            ((pltpu.VMEM((picks,) + tile_shape, BF16),) if owner else ())
            + (pltpu.SemaphoreType.DMA((picks,)),) * (1 + owner),
            60 * 1024 * 1024 if owner else VMEM_LIMIT,
        )

    incoming = lax.ppermute(gathered(1, "gather_out"), "frame", [(0, 1), (1, 0)])
    own = gathered(0, "gather_own")
    pairs = lax.dynamic_slice_in_dim(ref_pairs, group * frames, frames, 0)
    slot_range = jnp.arange(ref_slots.shape[0], dtype=jnp.int32)
    slots = jnp.sum(jnp.where(pairs[:, :, None] == slot_range, ref_slots, 0), axis=-1)
    held = slots // local_refs == group
    picked = jnp.where(
        held[:, :, None, None, None],
        own.reshape(frames, 2, channels, rows, width),
        incoming.reshape(frames, 2, channels, rows, width),
    )
    xr = picked.transpose(0, 3, 1, 2, 4).reshape(frames, rows, 2 * channels, width)
    xc = current_frames.transpose(0, 2, 1, 3)

    jk = join_kernel.reshape(3 * taps, joined)
    ok = out_kernel.reshape(3 * taps, channels)
    prepared = [
        struct((taps, 3 * joined), BF16),
        struct((taps, taps), BF16),
        struct((taps, taps), BF16),
        struct((3 * taps, channels), BF16),
    ]
    w1, w2, w3, back = run(
        prepare_body, "prepare", (), (jk, ok), [whole(jk), whole(ok)], prepared,
        [whole(x) for x in prepared], (1,), 4 * jk.size, 4 * (jk.size + 3 * ok.size),
    )

    mid = (frames, rows - 2, channels, width)
    line = (frames, channels, width)
    mid_b, mid_f = struct(mid, BF16), struct(mid, F32)
    line_b, line_f = struct(line, BF16), struct(line, F32)
    edge_bytes = 24 * frames * channels * width
    mid_bytes = 10 * frames * rows * channels * width
    edge_flops = conv_flops * channels // (3 * rows) * 2

    up, down = run(
        edge_taps_body, "edge_taps", (), (xr, xc, xr, xc, jk),
        [row(xr, 0), row(xc, 0), row(xr, rows - 1), row(xc, rows - 1), whole(jk)],
        [line_b] * 2, [whole(line_b)] * 2, (1,), 3 * edge_flops, edge_bytes,
    )
    above, below = swap_edges(up, down, "tile")

    outs = [mid_b, mid_f, line_f, line_f]
    hm, sm, top, bottom = run(
        join_body, "join_conv", (), (xr, xc, w1), [each(xr), each(xc), whole(w1)],
        outs, [each(x) for x in outs], (frames,), conv_flops * joined, mid_bytes,
    )
    ht, hb, st, sb = run(
        functools.partial(join_edge_body, count=count), "join_edge", (tile_id,),
        (top, bottom, below, above), [whole(line_f)] * 4,
        [line_b, line_b, line_f, line_f], [whole(line_f)] * 4, (1,), edge_bytes, edge_bytes,
    )
    h_above, h_below = swap_edges(ht, hb, "tile")

    rated = (frame_numbers, rate_weights, group_id)
    outs = [mid_b, mid_b, line_f, line_f, struct((frames, 8, width), F32)]
    cm, rm, top, bottom, scales = run(
        functools.partial(output_body, cells=cells, frames=frames), "out_conv", rated,
        (hm, ht, hb, xc, w2), [each(x) for x in (hm, ht, hb, xc)] + [whole(w2)],
        outs, [each(x) for x in outs], (frames,), conv_flops * channels, mid_bytes,
    )
    ct, cb, rt, rb = run(
        functools.partial(output_edge_body, count=count),
        "out_edge", (tile_id,), (top, bottom, h_above, h_below, xc, xc, scales, ok),
        [whole(line_f)] * 4 + [row(xc, 0), row(xc, rows - 1), whole(scales), whole(ok)],
        [line_b] * 4, [whole(line_b)] * 4, (1,), edge_flops, edge_bytes,
    )
    r_above, r_below = swap_edges(rt, rb, "tile")

    outs = [mid_b, line_f, line_f]
    gm, top, bottom = run(
        slope_body, "back_conv", (), (rm, rt, rb, sm, w3),
        [each(x) for x in (rm, rt, rb, sm)] + [whole(w3)],
        outs, [each(x) for x in outs], (frames,), conv_flops * channels, mid_bytes,
    )
    og_s = struct((taps, taps), F32)
    og = run(
        out_grad_body, "out_grad", (), (hm, ht, hb, rm, rt, rb),
        [each(x) for x in (hm, ht, hb, rm, rt, rb)], og_s, whole(og_s), (frames,),
        conv_flops * channels, mid_bytes,
    )
    recon = jnp.concatenate([ct[:, None], cm, cb[:, None]], 1).transpose(0, 2, 1, 3)
    recon = with_layout_constraint(recon, Layout((0, 1, 2, 3)))
    gt, gb = run(
        functools.partial(slope_edge_body, count=count), "back_edge", (tile_id,),
        (top, bottom, r_above, r_below, st, sb, back), [whole(line_f)] * 6 + [whole(back)],
        [line_b] * 2, [whole(line_b)] * 2, (1,), edge_flops, edge_bytes,
    )
    g_above, g_below = swap_edges(gt, gb, "tile")

    near = 4 if count % 4 == 0 else count
    unit = 16 * 2 * near
    packed_rows = 3 * taps * (joined + channels) // LANES
    packed_s = struct((pl.cdiv(packed_rows, unit) * unit, LANES), F32)
    half_s = struct((packed_s.shape[0] // 2, LANES), F32)
    args = (gm, gt, gb, xr, xc, ht, hb, r_above, r_below)
    packed = run(
        functools.partial(grads_body, count=count), "grads", (tile_id,), args + (og,),
        [each(x) for x in args] + [whole(og)], packed_s, whole(packed_s), (frames,),
        conv_flops * joined, 2 * mid_bytes,
    )
    send, part = run(
        functools.partial(grads_edge_body, count=count), "grads_edge", (tile_id, group_id),
        (packed, g_above, g_below, xr, xc, xr, xc),
        [whole(packed_s), whole(line_b), whole(line_b)]
        + [row(xr, 0), row(xc, 0), row(xr, rows - 1), row(xc, rows - 1)],
        [struct(half_s.shape, BF16), half_s], [whole(half_s)] * 2, (1,), 3 * edge_flops, edge_bytes,
        (pltpu.VMEM(packed_s.shape, F32),),
    )
    part = part + lax.ppermute(send, "frame", [(0, 1), (1, 0)]).astype(F32)
    me = lax.axis_index("tile") % near
    size = part.shape[0] // near

    def trade(x, mask):
        return lax.ppermute(x, "tile", [(i, i ^ mask) for i in range(count)])

    def quarter(mask):
        return lax.dynamic_slice_in_dim(part, (me ^ mask) * size, size, 0)

    gots = [trade(quarter(mask).astype(BF16), mask) for mask in range(1, near)]
    total = quarter(0)
    for got in gots:
        total = total + got.astype(F32)
    total = total.astype(BF16)
    mask = near
    while mask < count:
        total = (total.astype(F32) + trade(total, mask).astype(F32)).astype(BF16)
        mask *= 2
    total, recon = lax.optimization_barrier((total, recon))
    pieces = [total] + [trade(total, mask) for mask in range(1, near)]
    others = [lax.ppermute(x, "frame", [(0, 1), (1, 0)]) for x in pieces]
    outs = [struct(join_kernel.shape, F32), struct(out_kernel.shape, F32)]
    join_total, out_total = run(
        functools.partial(unpack_body, near=near), "unpack", (group_id, tile_id), (*pieces, *others),
        [whole(x) for x in pieces + others],
        outs, [whole(x) for x in outs], (1,), 0, 8 * packed_s.size,
        (pltpu.VMEM(packed_s.shape, F32),),
    )
    return recon, join_total, out_total


def solution(mesh):
    placed = (
        P(("parts", "frame"), None, "tile", None),
        P(("parts", "frame"), None, "tile", None),
        P("parts", None),
        P("parts"),
        P("parts"),
        P("parts"),
        P(),
        P(),
    )
    return jax.shard_map(
        on_device,
        mesh=mesh,
        in_specs=placed,
        out_specs=(
            P(("parts", "frame"), None, "tile", None),
            P("parts", None, None, None),
            P("parts", None, None, None),
        ),
        check_vma=False,
    )
```

```python
import functools

import jax
import jax.numpy as jnp
from jax import lax
from jax.experimental.layout import Layout, with_layout_constraint
from jax.experimental import pallas as pl
from jax.experimental.pallas import tpu as pltpu
from jax.sharding import PartitionSpec as P

F32 = jnp.float32
BF16 = jnp.bfloat16
LANES = 128
VMEM_LIMIT = 16 * 1024 * 1024


def call(body, name, flops, nbytes, vmem, **kw):
    return pl.pallas_call(
        body,
        name=name,
        cost_estimate=pl.CostEstimate(flops=flops, bytes_accessed=nbytes, transcendentals=0),
        compiler_params=pltpu.CompilerParams(vmem_limit_bytes=vmem),
        **kw,
    )


def whole_spec(shape):
    return pl.BlockSpec(shape, lambda *_: (0,) * len(shape))


def from_left(x):
    lane = lax.broadcasted_iota(jnp.int32, x.shape, 1)
    return jnp.where(lane == 0, jnp.zeros((), x.dtype), pltpu.roll(x, 1, 1))


def from_right(x):
    lane = lax.broadcasted_iota(jnp.int32, x.shape, 1)
    w = x.shape[1]
    return jnp.where(lane == w - 1, jnp.zeros((), x.dtype), pltpu.roll(x, w - 1, 1))


def shift_sum(y):
    c = y.shape[0] // 3
    return y[c : 2 * c] + from_left(y[:c]) + from_right(y[2 * c :])


def conv_rows(weights, rows, width, group=2):
    zero = jnp.zeros_like(rows[0])
    padded = [zero] + rows + [zero]
    sums = []
    for r0 in range(0, len(rows), group):
        columns = [
            jnp.concatenate(padded[r : r + 3], 0) for r in range(r0, min(r0 + group, len(rows)))
        ]
        y = jnp.dot(weights, jnp.concatenate(columns, 1), preferred_element_type=F32)
        for j in range(len(columns)):
            sums.append(shift_sum(y[:, j * width : (j + 1) * width]))
    return sums


def gather_body(pairs, slots, group, refs, out, *scratch, owner, frames):
    local_refs = refs.shape[0]
    picks = out.shape[0]
    g = group[0]
    wanted = (g if owner == 0 else 1 - g) * frames
    tiles, sems = (out, scratch[0]) if owner == 0 else scratch[:2]

    def fetch(i):
        slot = slots[pairs[i % 2, wanted + i // 2]] - g * local_refs
        slot = jnp.clip(slot, 0, local_refs - 1)
        return pltpu.make_async_copy(refs.at[slot], tiles.at[i], sems.at[i])

    def put(i):
        return pltpu.make_async_copy(tiles.at[i], out.at[i], scratch[2].at[i])

    for i in range(picks):
        fetch(i).start()
    for i in range(picks):
        fetch(i).wait()
        if owner:
            put(i).start()
    if owner:
        for i in range(picks):
            put(i).wait()


def prepare_body(jk, ok, w1, w2, w3, back):
    channels = ok.shape[1]
    taps = 3 * channels
    w1[...] = jnp.concatenate([jk[p * taps : (p + 1) * taps, :] for p in range(3)], 1)
    w2[...] = jnp.concatenate([ok[p * taps : (p + 1) * taps, :] for p in range(3)], 1)
    blocks = []
    for p in range(3):
        rows = []
        for q in range(3):
            at = ((2 - p) * 3 + 2 - q) * channels
            rows.append(ok[at : at + channels, :].astype(F32).T.astype(BF16))
        blocks.append(jnp.concatenate(rows, 0))
        back[p * taps : (p + 1) * taps, :] = blocks[-1]
    w3[...] = jnp.concatenate(blocks, 1)


def inside(tile, count, above, below):
    t = tile[0]
    return jnp.where(t > 0, above, jnp.zeros_like(above)), jnp.where(
        t < count - 1, below, jnp.zeros_like(below)
    )


def edge_sums(w, p, cells):
    taps = w.shape[0] // 3
    width = cells[0].shape[1]
    y = jnp.dot(
        w[p * taps : (p + 1) * taps, :],
        jnp.concatenate(cells, 1),
        preferred_element_type=F32,
    )
    return [shift_sum(y[:, k * width : (k + 1) * width]) for k in range(len(cells))]


def edge_taps_body(xr0, xc0, xr1, xc1, w, up, down):
    frames = up.shape[0]
    for xr, xc, p, out in ((xr0, xc0, 2, up), (xr1, xc1, 0, down)):
        cells = [jnp.concatenate([xr[b, 0], xc[b, 0]], 0) for b in range(frames)]
        for b, x in enumerate(edge_sums(w, p, cells)):
            out[b] = x.astype(BF16)


def silu_and_slope(v):
    s = jax.nn.sigmoid(v)
    return (v * s).astype(BF16), s * (1.0 + v * (1.0 - s))


def join_body(xr, xc, w, hidden, slope, top, bottom):
    rows, width = xr.shape[1], xr.shape[3]
    stacked = [jnp.concatenate([xr[0, r], xc[0, r]], 0) for r in range(rows)]
    sums = conv_rows(w[...], stacked, width)
    top[0] = sums[0]
    bottom[0] = sums[-1]
    for r in range(1, rows - 1):
        hidden[0, r - 1], slope[0, r - 1] = silu_and_slope(sums[r])


def join_edge_body(tile, top, bottom, below, above, ht, hb, st, sb, *, count):
    for b in range(top.shape[0]):
        got_a, got_b = inside(tile, count, above[b].astype(F32), below[b].astype(F32))
        ht[b], st[b] = silu_and_slope(top[b] + got_a)
        hb[b], sb[b] = silu_and_slope(bottom[b] + got_b)


def frame_scale(numbers, rates, group, cells, b, frames):
    return rates[numbers[group[0] * frames + b]] * (2.0 / cells)


def column(first, mid, last):
    return [first[0]] + [mid[0, r] for r in range(mid.shape[1])] + [last[0]]


def output_body(
    numbers, rates, group, hm, ht, hb, xc, w, recon, residual, top, bottom, scales,
    *, cells, frames
):
    hidden = column(ht, hm, hb)
    sums = conv_rows(w[...], hidden, hm.shape[3])
    scale = frame_scale(numbers, rates, group, cells, pl.program_id(0), frames)
    top[0] = sums[0]
    bottom[0] = sums[-1]
    scales[0] = jnp.full(scales.shape[1:], scale, F32)
    for r in range(1, len(sums) - 1):
        recon[0, r - 1] = sums[r].astype(BF16)
        residual[0, r - 1] = ((sums[r] - xc[0, r].astype(F32)) * scale).astype(BF16)


def output_edge_body(
    tile, top, bottom, above, below, xc0, xc1, scales, w, ct, cb, rt, rb, *, count
):
    frames = top.shape[0]
    got = inside(tile, count, above[...], below[...])
    for g, p, part, xc, c, r in (
        (got[0], 0, top, xc0, ct, rt),
        (got[1], 2, bottom, xc1, cb, rb),
    ):
        for b, x in enumerate(edge_sums(w, p, [g[b] for b in range(frames)])):
            total = part[b] + x
            c[b] = total.astype(BF16)
            r[b] = ((total - xc[b, 0].astype(F32)) * scales[b, :1, :]).astype(BF16)


def slope_body(rm, rt, rb, slope, w, grad, top, bottom):
    sums = conv_rows(w[...], column(rt, rm, rb), rm.shape[3])
    top[0] = sums[0]
    bottom[0] = sums[-1]
    for r in range(1, len(sums) - 1):
        grad[0, r - 1] = (sums[r] * slope[0, r - 1]).astype(BF16)


def slope_edge_body(tile, top, bottom, above, below, st, sb, w, gt, gb, *, count):
    got = inside(tile, count, above[...], below[...])
    for g, p, part, slope, grad in ((got[0], 0, top, st, gt), (got[1], 2, bottom, sb, gb)):
        for b, x in enumerate(edge_sums(w, p, [g[b] for b in range(g.shape[0])])):
            grad[b] = ((part[b] + x) * slope[b]).astype(BF16)


def contract(left, right):
    return lax.dot_general(left, right, (((1,), (1,)), ((), ())), preferred_element_type=F32)


def lane_blocks(x):
    return [x[:, k : k + LANES] for k in range(0, x.shape[1], LANES)]


def add_up(out, value):
    first = pl.program_id(0) == 0

    @pl.when(first)
    def _():
        out[...] = value

    @pl.when(jnp.logical_not(first))
    def _():
        out[...] += value


def side_taps(rows):
    return [[from_left(x) for x in rows], rows, [from_right(x) for x in rows]]


def out_grad_body(hm, ht, hb, rm, rt, rb, out):
    hidden = side_taps(column(ht, hm, hb))
    residual = column(rt, rm, rb)
    zero = jnp.zeros_like(residual[0])
    padded = [zero] + residual + [zero]
    rows = len(residual)
    value = contract(
        jnp.concatenate(
            [jnp.concatenate(padded[2 - p : 2 - p + rows], 1) for p in range(3)], 0
        ),
        jnp.concatenate([jnp.concatenate(h, 1) for h in hidden], 0),
    )
    add_up(out, value)


def grads_body(tile, gm, gt, gb, xr, xc, ht, hb, above, below, og, packed, *, count):
    rows, width = xr.shape[1], xr.shape[3]
    channels = gm.shape[2]
    joined = xr.shape[2] + xc.shape[2]
    rest = joined % 256
    head = joined - rest
    zero = jnp.zeros((channels, width), BF16)
    turned = side_taps(column(gt, gm, gb))[::-1]
    stacked = [jnp.concatenate([xr[0, r], xc[0, r]], 0) for r in range(rows)]
    taps = []
    for p in range(3):
        for q in range(3):
            taps.append(
                jnp.concatenate(
                    [turned[q][r - p + 1] if 0 <= r - p + 1 < rows else zero for r in range(rows)],
                    1,
                )
            )
    main = contract(jnp.concatenate(taps, 0), jnp.concatenate([s[:head] for s in stacked], 1))
    tails = [s[head:] for s in stacked]
    tail_zero = jnp.zeros_like(tails[0])
    tail = contract(
        jnp.concatenate([jnp.concatenate(turned[q], 1) for q in range(3)], 0),
        jnp.concatenate(
            [
                jnp.concatenate(
                    [tails[r + p - 1] if 0 <= r + p - 1 < rows else tail_zero for r in range(rows)],
                    1,
                )
                for p in range(3)
            ],
            0,
        ),
    )
    got = inside(tile, count, above[0], below[0])
    out = jnp.concatenate(
        [
            contract(got[1], jnp.concatenate([x[0] for x in side_taps([hb[0]])], 0)),
            jnp.zeros((channels, 3 * channels), F32),
            contract(got[0], jnp.concatenate([x[0] for x in side_taps([ht[0]])], 0)),
        ],
        0,
    )
    first = pl.program_id(0) == 0
    out = out + jnp.where(first, og[...], 0.0)
    blocks = lane_blocks(main) + lane_blocks(jnp.concatenate([out, tail], 1))

    @pl.when(first)
    def _():
        at = 0
        for block in blocks:
            packed[at : at + block.shape[0], :] = block
            at += block.shape[0]
        if at < packed.shape[0]:
            packed[at:, :] = jnp.zeros((packed.shape[0] - at, LANES), F32)

    @pl.when(jnp.logical_not(first))
    def _():
        at = 0
        for block in blocks:
            packed[at : at + block.shape[0], :] += block
            at += block.shape[0]


def grads_edge_body(
    tile, group, packed_in, above, below, xr0, xc0, xr1, xc1, send, keep, packed, *, count
):
    frames, channels, _ = above.shape
    joined = xr0.shape[2] + xc0.shape[2]
    rest = joined % 256
    head = joined - rest
    taps = 3 * channels
    half = send.shape[0]
    packed[...] = packed_in[...]
    tail_at = 3 * taps * (head // LANES)
    got = inside(tile, count, above[...], below[...])
    for p, edge, xr, xc in ((2, got[0], xr0, xc0), (0, got[1], xr1, xc1)):
        rows = [edge[b] for b in range(frames)]
        left = jnp.concatenate(
            [
                jnp.concatenate([move(g) for g in rows], 1)
                for move in (from_right, lambda g: g, from_left)
            ],
            0,
        )
        right = jnp.concatenate(
            [jnp.concatenate([xr[b, 0], xc[b, 0]], 0) for b in range(frames)], 1
        )
        extra = contract(left, right)
        for k, block in enumerate(lane_blocks(extra[:, :head])):
            at = 3 * taps * k + taps * p
            packed[at : at + taps, :] += block
        lane = taps + rest * p
        at = tail_at + taps * (lane // LANES)
        lane = lane % LANES
        packed[at : at + taps, lane : lane + rest] += extra[:, head:]
    g = group[0]
    send[...] = packed[pl.ds(pl.multiple_of((1 - g) * half, 8), half), :].astype(BF16)
    keep[...] = packed[pl.ds(pl.multiple_of(g * half, 8), half), :]


def unpack_body(group, tile, *refs, near):
    own, got, (join, out, packed) = refs[:near], refs[near : 2 * near], refs[2 * near :]
    channels = out.shape[2]
    joined = join.shape[3]
    rest = joined % 256
    head = joined - rest
    taps = 3 * channels
    size = own[0].shape[0]
    half = near * size
    g = group[0]
    me = lax.rem(tile[0], near)
    for k in range(near):
        at = (me ^ k) * size
        for held, x in ((g, own), (1 - g, got)):
            packed[pl.ds(pl.multiple_of(held * half + at, 8), size), :] = x[k][
                ...
            ].astype(F32)
    tail_at = 3 * taps * (head // LANES)
    tail = jnp.concatenate(
        [
            packed[tail_at + taps * k : tail_at + taps * (k + 1), :]
            for k in range((taps + 3 * rest) // LANES)
        ],
        1,
    )
    for p in range(3):
        for q in range(3):
            rows = slice(q * channels, (q + 1) * channels)
            at = taps * p + q * channels
            pieces = [
                packed[3 * taps * k + at : 3 * taps * k + at + channels, :]
                for k in range(head // LANES)
            ]
            pieces.append(tail[rows, taps + rest * p : taps + rest * (p + 1)])
            join[p, q] = jnp.concatenate(pieces, 1)
            out[p, q] = tail[p * channels : (p + 1) * channels, q * channels : (q + 1) * channels]


def swap_edges(up, down, axis):
    count = lax.axis_size(axis)
    below = lax.ppermute(up, axis, [((i + 1) % count, i) for i in range(count)])
    above = lax.ppermute(down, axis, [(i, (i + 1) % count) for i in range(count)])
    return above, below


def on_device(
    decoded_refs,
    current_frames,
    ref_pairs,
    ref_slots,
    frame_numbers,
    rate_weights,
    join_kernel,
    out_kernel,
):
    local_refs = decoded_refs.shape[0]
    frames, channels, rows, width = current_frames.shape
    joined = join_kernel.shape[3]
    count = lax.axis_size("tile")
    cells = rows * count * width
    group = lax.axis_index("frame")
    group_id = group.reshape(1).astype(jnp.int32)
    tile_id = lax.axis_index("tile").reshape(1).astype(jnp.int32)
    picks = 2 * frames
    taps = 3 * channels
    conv_flops = 2 * frames * rows * width * 3 * taps

    def struct(shape, dtype):
        return jax.ShapeDtypeStruct(shape, dtype)

    def run(
        body, name, scalars, args, specs, outs, out_specs, grid, flops, nbytes, scratch=(),
        vmem=VMEM_LIMIT,
    ):
        return call(
            body,
            name,
            flops,
            nbytes,
            vmem,
            grid_spec=pltpu.PrefetchScalarGridSpec(
                num_scalar_prefetch=len(scalars),
                grid=grid,
                in_specs=specs,
                out_specs=out_specs,
                scratch_shapes=scratch,
            ),
            out_shape=outs,
        )(*scalars, *args)

    def each(x):
        return pl.BlockSpec((1,) + x.shape[1:], lambda b, *_: (b,) + (0,) * (len(x.shape) - 1))

    def whole(x):
        return whole_spec(x.shape)

    def row(x, r):
        return pl.BlockSpec((frames, 1) + x.shape[2:], lambda *_: (0, r, 0, 0))

    pairs_of = ref_pairs.T
    tile_shape = decoded_refs.shape[1:]

    def gathered(owner, name):
        return run(
            functools.partial(gather_body, owner=owner, frames=frames),
            name,
            (pairs_of, ref_slots, group_id),
            (pltpu.with_memory_space_constraint(decoded_refs, pltpu.HBM),),
            [pl.BlockSpec(memory_space=pltpu.HBM)],
            struct((picks,) + tile_shape, BF16),
            pl.BlockSpec(memory_space=pltpu.HBM if owner else pltpu.VMEM),
            (1,),
            0,
            4 * picks * channels * rows * width,
            ((pltpu.VMEM((picks,) + tile_shape, BF16),) if owner else ())
            + (pltpu.SemaphoreType.DMA((picks,)),) * (1 + owner),
            60 * 1024 * 1024 if owner else VMEM_LIMIT,
        )

    incoming = lax.ppermute(gathered(1, "gather_out"), "frame", [(0, 1), (1, 0)])
    own = gathered(0, "gather_own")
    pairs = lax.dynamic_slice_in_dim(ref_pairs, group * frames, frames, 0)
    slot_range = jnp.arange(ref_slots.shape[0], dtype=jnp.int32)
    slots = jnp.sum(jnp.where(pairs[:, :, None] == slot_range, ref_slots, 0), axis=-1)
    held = slots // local_refs == group
    picked = jnp.where(
        held[:, :, None, None, None],
        own.reshape(frames, 2, channels, rows, width),
        incoming.reshape(frames, 2, channels, rows, width),
    )
    xr = picked.transpose(0, 3, 1, 2, 4).reshape(frames, rows, 2 * channels, width)
    xc = current_frames.transpose(0, 2, 1, 3)

    jk = join_kernel.reshape(3 * taps, joined)
    ok = out_kernel.reshape(3 * taps, channels)
    prepared = [
        struct((taps, 3 * joined), BF16),
        struct((taps, taps), BF16),
        struct((taps, taps), BF16),
        struct((3 * taps, channels), BF16),
    ]
    w1, w2, w3, back = run(
        prepare_body, "prepare", (), (jk, ok), [whole(jk), whole(ok)], prepared,
        [whole(x) for x in prepared], (1,), 4 * jk.size, 4 * (jk.size + 3 * ok.size),
    )

    mid = (frames, rows - 2, channels, width)
    line = (frames, channels, width)
    mid_b, mid_f = struct(mid, BF16), struct(mid, F32)
    line_b, line_f = struct(line, BF16), struct(line, F32)
    edge_bytes = 24 * frames * channels * width
    mid_bytes = 10 * frames * rows * channels * width
    edge_flops = conv_flops * channels // (3 * rows) * 2

    up, down = run(
        edge_taps_body, "edge_taps", (), (xr, xc, xr, xc, jk),
        [row(xr, 0), row(xc, 0), row(xr, rows - 1), row(xc, rows - 1), whole(jk)],
        [line_b] * 2, [whole(line_b)] * 2, (1,), 3 * edge_flops, edge_bytes,
    )
    above, below = swap_edges(up, down, "tile")

    outs = [mid_b, mid_f, line_f, line_f]
    hm, sm, top, bottom = run(
        join_body, "join_conv", (), (xr, xc, w1), [each(xr), each(xc), whole(w1)],
        outs, [each(x) for x in outs], (frames,), conv_flops * joined, mid_bytes,
    )
    ht, hb, st, sb = run(
        functools.partial(join_edge_body, count=count), "join_edge", (tile_id,),
        (top, bottom, below, above), [whole(line_f)] * 4,
        [line_b, line_b, line_f, line_f], [whole(line_f)] * 4, (1,), edge_bytes, edge_bytes,
    )
    h_above, h_below = swap_edges(ht, hb, "tile")

    rated = (frame_numbers, rate_weights, group_id)
    outs = [mid_b, mid_b, line_f, line_f, struct((frames, 8, width), F32)]
    cm, rm, top, bottom, scales = run(
        functools.partial(output_body, cells=cells, frames=frames), "out_conv", rated,
        (hm, ht, hb, xc, w2), [each(x) for x in (hm, ht, hb, xc)] + [whole(w2)],
        outs, [each(x) for x in outs], (frames,), conv_flops * channels, mid_bytes,
    )
    ct, cb, rt, rb = run(
        functools.partial(output_edge_body, count=count),
        "out_edge", (tile_id,), (top, bottom, h_above, h_below, xc, xc, scales, ok),
        [whole(line_f)] * 4 + [row(xc, 0), row(xc, rows - 1), whole(scales), whole(ok)],
        [line_b] * 4, [whole(line_b)] * 4, (1,), edge_flops, edge_bytes,
    )
    r_above, r_below = swap_edges(rt, rb, "tile")

    outs = [mid_b, line_f, line_f]
    gm, top, bottom = run(
        slope_body, "back_conv", (), (rm, rt, rb, sm, w3),
        [each(x) for x in (rm, rt, rb, sm)] + [whole(w3)],
        outs, [each(x) for x in outs], (frames,), conv_flops * channels, mid_bytes,
    )
    og_s = struct((taps, taps), F32)
    og = run(
        out_grad_body, "out_grad", (), (hm, ht, hb, rm, rt, rb),
        [each(x) for x in (hm, ht, hb, rm, rt, rb)], og_s, whole(og_s), (frames,),
        conv_flops * channels, mid_bytes,
    )
    recon = jnp.concatenate([ct[:, None], cm, cb[:, None]], 1).transpose(0, 2, 1, 3)
    recon = with_layout_constraint(recon, Layout((0, 1, 2, 3)))
    gt, gb = run(
        functools.partial(slope_edge_body, count=count), "back_edge", (tile_id,),
        (top, bottom, r_above, r_below, st, sb, back), [whole(line_f)] * 6 + [whole(back)],
        [line_b] * 2, [whole(line_b)] * 2, (1,), edge_flops, edge_bytes,
    )
    g_above, g_below = swap_edges(gt, gb, "tile")

    near = 4 if count % 4 == 0 else count
    unit = 8 * 2 * near
    packed_rows = 3 * taps * (joined + channels) // LANES
    packed_s = struct((pl.cdiv(packed_rows, unit) * unit, LANES), F32)
    half_s = struct((packed_s.shape[0] // 2, LANES), F32)
    args = (gm, gt, gb, xr, xc, ht, hb, r_above, r_below)
    packed = run(
        functools.partial(grads_body, count=count), "grads", (tile_id,), args + (og,),
        [each(x) for x in args] + [whole(og)], packed_s, whole(packed_s), (frames,),
        conv_flops * joined, 2 * mid_bytes,
    )
    send, part = run(
        functools.partial(grads_edge_body, count=count), "grads_edge", (tile_id, group_id),
        (packed, g_above, g_below, xr, xc, xr, xc),
        [whole(packed_s), whole(line_b), whole(line_b)]
        + [row(xr, 0), row(xc, 0), row(xr, rows - 1), row(xc, rows - 1)],
        [struct(half_s.shape, BF16), half_s], [whole(half_s)] * 2, (1,), 3 * edge_flops, edge_bytes,
        (pltpu.VMEM(packed_s.shape, F32),),
    )
    part = part + lax.ppermute(send, "frame", [(0, 1), (1, 0)]).astype(F32)
    me = lax.axis_index("tile") % near
    size = part.shape[0] // near

    def trade(x, mask):
        return lax.ppermute(x, "tile", [(i, i ^ mask) for i in range(count)])

    def quarter(mask):
        return lax.dynamic_slice_in_dim(part, (me ^ mask) * size, size, 0)

    gots = [trade(quarter(mask).astype(BF16), mask) for mask in range(1, near)]
    total = quarter(0)
    for got in gots:
        total = total + got.astype(F32)
    total = total.astype(BF16)
    mask = near
    while mask < count:
        total = (total.astype(F32) + trade(total, mask).astype(F32)).astype(BF16)
        mask *= 2
    total, recon = lax.optimization_barrier((total, recon))
    pieces = [total] + [trade(total, mask) for mask in range(1, near)]
    others = [lax.ppermute(x, "frame", [(0, 1), (1, 0)]) for x in pieces]
    outs = [struct(join_kernel.shape, F32), struct(out_kernel.shape, F32)]
    join_total, out_total = run(
        functools.partial(unpack_body, near=near), "unpack", (group_id, tile_id), (*pieces, *others),
        [whole(x) for x in pieces + others],
        outs, [whole(x) for x in outs], (1,), 0, 8 * packed_s.size,
        (pltpu.VMEM(packed_s.shape, F32),),
    )
    return recon, join_total, out_total


def solution(mesh):
    placed = (
        P(("parts", "frame"), None, "tile", None),
        P(("parts", "frame"), None, "tile", None),
        P("parts", None),
        P("parts"),
        P("parts"),
        P("parts"),
        P(),
        P(),
    )
    return jax.shard_map(
        on_device,
        mesh=mesh,
        in_specs=placed,
        out_specs=(
            P(("parts", "frame"), None, "tile", None),
            P("parts", None, None, None),
            P("parts", None, None, None),
        ),
        check_vma=False,
    )
```
